512 devices in a mesh: ens: 4 (over y_hi), lat: 2 (over core), lon: 64 (over y_lo, z, x).
Axes of the slice: x: 4, y: 8 (y_hi: 4, y_lo: 2; y = y_hi * 2 + y_lo), z: 8, core: 2. Of those that a mesh axis runs over, the one named last changes fastest.
Arguments:
- fields: bfloat16 [8, 36, 1536, 384], P('ens', 'lat', 'lon'), parts along dimension 0, may hold values from -6 to 6
- region_ids: int32 [2, 36, 1536], P(None, 'lat', 'lon'), may hold values from 0 to 3
- bias_index: int32 [144, 144], replicated, may hold values from 0 to 3311
- earth_bias: bfloat16 [6, 3312, 12], P('lat'), may hold values from -70 to 170
- w_qkv: bfloat16 [384, 1152], replicated, may hold values from -0.3125 to 0.3125
- w_proj: bfloat16 [384, 384], replicated, may hold values from -0.3125 to 0.3125
- w_fc1: bfloat16 [384, 1536], replicated, may hold values from -0.3125 to 0.3125
- w_fc2: bfloat16 [1536, 384], replicated, may hold values from -0.15625 to 0.15625
Outputs:
- result: bfloat16 [8, 36, 1536, 384], P('ens', 'lat', 'lon'), parts along dimension 0
The draws below stay inside these ranges and needn't reach their ends.
There are 4 independent parts, one for each index of `ens`. The reference program is written for one: setup_inputs(seed, part) draws one part's arguments, and reference() takes and returns one part's arrays. A program takes and returns all parts, laid end to end along the dimension named above; an argument that names none is the same for every part. Nothing has to cross between parts.
All inputs are finite; a program needn't handle non-finite values.
Results may differ from the reference program's by a relative error of at most 0.009.
Values may be sent and summed in bfloat16 or wider, within the bound.
No kernel may reach another device: no remote copies, remote signals or barrier semaphores. Data moves between devices by JAX's collectives and lax.ppermute only.
A program may use at most 128 MiB of HBM per device.

```python
import jax
import jax.numpy as jnp
from jax import lax

C = 384
HEADS = 12
FFH = 1536
WZ = 2
WLAT = 6
WLON = 12
LEV = 2
WIN_TOK = 144
BIAS_POS = 3312
NLAT = 36
NLON = 1536
LATW = 6


def draw_earth_bias(key, part):
    key_base, key_offset = jax.random.split(jax.random.fold_in(key, 17))
    table_shape = (LATW, BIAS_POS, HEADS)
    values = jnp.clip(jax.random.normal(key_base, table_shape, jnp.float32), -4.0, 4.0)
    return values.astype(jnp.bfloat16)


def with_ends(drawn, rng, low, largest):
    spot = [jax.random.randint(jax.random.fold_in(rng, axis), (), 0, length) for axis, length in enumerate(drawn.shape)]
    widest = drawn.shape.index(max(drawn.shape))
    beside = spot[:widest] + [(spot[widest] + 1) % drawn.shape[widest]] + spot[widest + 1:]
    return drawn.at[tuple(spot)].set(low).at[tuple(beside)].set(largest)


def block_scale(rng, extent, pieces, smallest, largest):
    def one(axis_at, shards_of):
        steps = jax.random.uniform(jax.random.fold_in(jax.random.fold_in(rng, 6), axis_at), (shards_of,), jnp.float32, smallest / len(pieces), largest / len(pieces))
        return jnp.repeat(jnp.exp(steps), extent[axis_at] // shards_of).reshape((-1,) + (1,) * (len(extent) - axis_at - 1))

    gain = one(*pieces[0])
    for cut in pieces[1:]:
        gain = gain * one(*cut)
    return gain


def normal_values(stream_key, extent, scale, reach, cuts=(), dtype=jnp.bfloat16):
    drawn = jax.random.normal(stream_key, extent, jnp.float32) * scale
    if len(cuts) > 0:
        drawn = block_scale(stream_key, extent, cuts, -0.22, 0.18) * drawn
    return jnp.clip(drawn, min=-reach, max=reach).astype(dtype)


def setup_inputs(seed: int = 0, part: int = 0) -> dict:
    arg_keys = jax.random.split(jax.random.key(seed), 9)
    part_keys = jax.random.split(jax.random.fold_in(arg_keys[8], part), 9)
    fields = normal_values(part_keys[0], (LEV, NLAT, NLON, C), 1.0, 6.0, ((1, 2), (2, 64)))
    region_ids = with_ends(jax.random.randint(arg_keys[1], (LEV, NLAT, NLON), 0, 4), jax.random.fold_in(arg_keys[1], 1), 0, 3).astype(jnp.int32)
    bias_index = with_ends(jax.random.randint(arg_keys[2], (WIN_TOK, WIN_TOK), 0, BIAS_POS), jax.random.fold_in(arg_keys[2], 1), 0, BIAS_POS - 1).astype(jnp.int32)
    earth_bias = draw_earth_bias(jax.random.fold_in(arg_keys[8], 71), part)
    w_qkv = normal_values(arg_keys[4], (C, 3 * C), C ** -0.5, 0.3125)
    w_proj = normal_values(arg_keys[5], (C, C), C ** -0.5, 0.3125)
    w_fc1 = normal_values(arg_keys[6], (C, FFH), C ** -0.5, 0.3125)
    w_fc2 = normal_values(arg_keys[7], (FFH, C), FFH ** -0.5, 0.15625)
    return {"fields": fields, "region_ids": region_ids, "bias_index": bias_index, "earth_bias": earth_bias, "w_qkv": w_qkv, "w_proj": w_proj, "w_fc1": w_fc1, "w_fc2": w_fc2}


EPS_NORM = 1e-05

def layer_norm(tokens_in):
    widened = tokens_in.astype(jnp.float32)
    average = lax.optimization_barrier(jnp.mean(widened, axis=-1, keepdims=True))
    centred = widened - average
    spread = lax.optimization_barrier(jnp.mean(centred * centred, axis=-1, keepdims=True))
    return (centred * lax.rsqrt(spread + EPS_NORM)).astype(jnp.bfloat16)

def attend(normed, region_block, bias_block, bias_index, w_qkv, w_proj):
    levels, lat_rows, lon_cols, feature_width = normed.shape
    lat_wins = lat_rows // WLAT
    lon_wins = lon_cols // WLON
    window_tokens = levels * WLAT * WLON
    head_count = bias_block.shape[-1]
    head_dim = feature_width // head_count
    windowed = normed.reshape(levels, lat_wins, WLAT, lon_wins, WLON, feature_width)
    windowed = windowed.transpose(1, 3, 0, 2, 4, 5).reshape(-1, feature_width)
    packed = jnp.dot(windowed, w_qkv, preferred_element_type=jnp.float32).astype(jnp.bfloat16)
    packed = packed.reshape(lat_wins, lon_wins, window_tokens, 3, head_count, head_dim)
    queries = packed[:, :, :, 0].astype(jnp.float32)
    key_rows = packed[:, :, :, 1].astype(jnp.float32)
    value_rows = packed[:, :, :, 2].astype(jnp.float32)
    regions = region_block.reshape(levels, lat_wins, WLAT, lon_wins, WLON)
    regions = regions.transpose(1, 3, 0, 2, 4).reshape(lat_wins, lon_wins, window_tokens)
    bias_table = bias_block[:, bias_index, :].astype(jnp.float32).transpose(0, 3, 1, 2)
    scores = jnp.einsum('abihd,abjhd->abhij', queries, key_rows) * head_dim ** (-0.5) + bias_table[:, None]
    allowed = regions[:, :, :, None] == regions[:, :, None, :]
    scores = jnp.where(allowed[:, :, None], scores, -jnp.inf)
    maxima = lax.optimization_barrier(jnp.max(scores, axis=-1, keepdims=True))
    exponent = jnp.exp(scores - maxima)
    attn_weights = (exponent / lax.optimization_barrier(jnp.sum(exponent, axis=-1, keepdims=True))).astype(jnp.bfloat16)
    context = jnp.einsum('abhij,abjhd->abihd', attn_weights.astype(jnp.float32), value_rows)
    context = context.astype(jnp.bfloat16).reshape(-1, feature_width)
    projected = jnp.dot(context, w_proj, preferred_element_type=jnp.float32).astype(jnp.bfloat16)
    projected = projected.reshape(lat_wins, lon_wins, levels, WLAT, WLON, feature_width)
    return projected.transpose(2, 0, 3, 1, 4, 5).reshape(levels, lat_rows, lon_cols, feature_width)

def feed_forward(residual, w_fc1, w_fc2):
    feature_width = residual.shape[-1]
    normed = layer_norm(residual).reshape(-1, feature_width)
    hidden = jax.nn.gelu(jnp.dot(normed, w_fc1, preferred_element_type=jnp.float32), approximate=False)
    hidden = hidden.astype(jnp.bfloat16)
    summed = residual.reshape(-1, feature_width).astype(jnp.float32) + jnp.dot(hidden, w_fc2, preferred_element_type=jnp.float32)
    return summed.astype(jnp.bfloat16).reshape(residual.shape)

def reference(fields, region_ids, bias_index, earth_bias, w_qkv, w_proj, w_fc1, w_fc2):
    half_lev = WZ // 2
    half_lat = WLAT // 2
    half_lon = WLON // 2
    normed = layer_norm(fields)
    shifted = jnp.roll(normed, (-half_lev, -half_lat, -half_lon), axis=(0, 1, 2))
    blocks = shifted.reshape(LEV, LATW, WLAT, NLON, C).transpose(1, 0, 2, 3, 4)
    region_blocks = region_ids.reshape(LEV, LATW, WLAT, NLON).transpose(1, 0, 2, 3)

    def one_band(packed_in):
        lat_band, regions, bias_table = packed_in
        return attend(lat_band, regions, bias_table[None], bias_index, w_qkv, w_proj)
    outputs = lax.map(one_band, (blocks, region_blocks, earth_bias))
    attn_out = outputs.transpose(1, 0, 2, 3, 4).reshape(LEV, NLAT, NLON, C)
    returned = jnp.roll(attn_out, (half_lev, half_lat, half_lon), axis=(0, 1, 2))
    residual = (fields.astype(jnp.float32) + returned.astype(jnp.float32)).astype(jnp.bfloat16)
    return feed_forward(residual, w_fc1, w_fc2)
```

```python
import numpy as np
import jax
import jax.numpy as jnp
from jax import lax
from jax.experimental import pallas as pl
from jax.experimental.pallas import tpu as pltpu
from jax.sharding import PartitionSpec as P

F32 = jnp.float32
BF16 = jnp.bfloat16
EPS = 1e-05
LOG2E = 1.4426950408889634
C = 384
HEADS = 12
QUAD = 40
KEYS = 160
CHUNKS = 13
ROWS = 40
STRIDE = 40


def region_constants():
    lane = np.arange(512)
    p = lane % 256
    kk = p % 40
    valid = (p < 160) & (kk < 36)
    src_col = 12 * (lane // 256) + 6 * ((p % 80) // 40) + kk % 6
    lane_row = (kk // 18) * 6 + (p // 80) * 3 + (kk % 18) // 6
    cols = ((np.arange(24)[:, None] == src_col[None]) & valid[None]).astype(np.float32)
    row = np.arange(36)
    row_id = (row // 18) * 6 + row % 6
    keep = ((row_id[:, None] == lane_row[None]) & valid[None]).astype(np.float32)
    group = ((row[None] % 18) // 6 == np.arange(8)[:, None]).astype(np.float32)
    fill = np.where(valid, 0.0, -1.0).astype(np.float32)[None]
    return cols, keep, group, fill


def window_order(padded):
    spots = []
    for r2 in range(2):
        for c2 in range(2):
            for level in range(2):
                for r3 in range(3):
                    for c6 in range(6):
                        spots.append(level * 72 + (r2 * 3 + r3) * 12 + c2 * 6 + c6)
            if padded:
                spots += [-1] * 4
    return np.array(spots)


def index_constants(half):
    rows = window_order(False)[72 * half:72 * half + 72]
    pick = (rows[:, None] == np.arange(144)[None]).astype(np.float32)
    place = (np.arange(144)[:, None] == window_order(True)[None]).astype(np.float32)
    tile = (np.arange(32)[:, None] == (np.arange(256) % 32)[None]).astype(np.float32)
    keep = ((np.arange(72) % 8)[:, None] == (np.arange(256) // 32)[None]).astype(np.float32)
    gather = ((np.arange(72) // 8)[None] == np.arange(16)[:, None]).astype(np.float32)
    return pick, place, tile, keep, gather


def dot(a, b):
    return jnp.dot(a, b, preferred_element_type=F32)


def normalise(x):
    mean = jnp.mean(x, axis=-1, keepdims=True)
    centred = x - mean
    var = jnp.mean(centred * centred, axis=-1, keepdims=True)
    return (centred * lax.rsqrt(var + EPS)).astype(BF16)


def prep_body(fields, region, tab, cols, keep, group, fill, nq, comb, pay, xq):
    for cs in range(4):
        for rt in range(6):
            xq[rt, 40 * cs + 32:40 * cs + 40, :] = jnp.zeros((8, C), F32)

    def triple(rt, carry):
        for level in range(2):
            for r3 in range(3):
                x = fields[level * 18 + 3 * rt + r3].astype(F32)
                n = normalise(x).astype(F32)
                base = 6 * ((1 - level) * 3 + r3)
                for cs in range(4):
                    xq[rt, 40 * cs + base:40 * cs + base + 6, :] = n[6 * cs:6 * cs + 6, :]
        return carry

    lax.fori_loop(0, 6, triple, 0)
    reg = region[...].astype(F32).astype(BF16)
    spread = dot(reg, cols[...]) * keep[...]
    rows = dot(group[...], spread.astype(BF16)) + fill[...]
    comb[...] = rows
    nq[...] = xq[...].astype(BF16)
    pay[0:160, :] = xq[0].astype(BF16)
    pay[160:320, :] = xq[5].astype(BF16)
    last = jnp.concatenate([rows[2:3, 0:256], rows[2:3, 256:512], jnp.zeros((14, 256), F32)], axis=0)
    pay[320:336, 0:256] = last.astype(BF16)
    for c in range(CHUNKS):
        pay[336 + 16 * c:352 + 16 * c, 0:256] = tab[ROWS * c:ROWS * c + 16, :].astype(BF16)


def lon_body(nq, lat, comb, pay_r, pay_l, scr_r, scr_l):
    first = lat[160:320, :].astype(F32)
    final = lat[0:160, :].astype(F32)
    scr_r[0:40, :] = first[120:160, :]
    scr_l[0:40, :] = first[0:40, :]
    scr_r[280:320, :] = final[120:160, :]
    scr_l[280:320, :] = final[0:40, :]
    for rt in range(6):
        own = nq[rt].astype(F32)
        scr_r[40 * rt + 40:40 * rt + 80, :] = own[120:160, :]
        scr_l[40 * rt + 40:40 * rt + 80, :] = own[0:40, :]
    pay_r[0:320, :] = scr_r[...].astype(BF16)
    pay_l[...] = scr_l[...].astype(BF16)
    top = lat[320:336, 0:256].astype(F32)
    rows = jnp.concatenate([top[1:2, :], comb[0:3, 256:512], jnp.zeros((12, 256), F32)], axis=0)
    pay_r[320:336, 0:256] = rows.astype(BF16)


def bias_body(own_x, index, tab, swap, pick, place, tile, keep, gather, main, rem, tabs, lo_m, hi_m, lo_r, hi_r):
    for c in range(CHUNKS):
        tabs[ROWS * c:ROWS * c + ROWS, :] = tab[ROWS * c:ROWS * c + ROWS, :]
        if not own_x:
            tabs[ROWS * c:ROWS * c + 16, :] = swap[336 + 16 * c:352 + 16 * c, 0:256].astype(F32)
    idx = index[...]
    for part, m_ref, r_ref in ((idx & 255, lo_m, lo_r), (idx >> 8, hi_m, hi_r)):
        picked = dot(pick[...], part.astype(F32).astype(BF16)).astype(BF16)
        full = dot(picked, place[...])
        m_ref[...] = full[:, 0:128]
        wide = dot(full[:, 128:160].astype(BF16), tile[...]) * keep[...]
        r_ref[...] = dot(gather[...], wide.astype(BF16))
    table = tabs[...].astype(BF16)
    low = lax.broadcasted_iota(jnp.int32, (256, 256), 0).astype(F32)

    def look(lo, hi):
        hot = jnp.where(low == lo, 1.0, 0.0).astype(BF16)
        got = dot(table, hot)
        out = got[0:ROWS]
        for c in range(1, CHUNKS):
            out = jnp.where(hi == float(c), got[ROWS * c:ROWS * c + ROWS], out)
        return out * LOG2E

    def pair(step, carry):
        i = 2 * step
        lo = jnp.concatenate([lo_m[pl.ds(i, 1), :], lo_m[pl.ds(i + 1, 1), :]], axis=1)
        hi = jnp.concatenate([hi_m[pl.ds(i, 1), :], hi_m[pl.ds(i + 1, 1), :]], axis=1)
        out = look(lo, hi)
        spot = i + 4 * (i // 36)
        main[pl.ds(pl.multiple_of(spot * STRIDE, 8), ROWS), :] = out[:, 0:128]
        main[pl.ds(pl.multiple_of(spot * STRIDE + STRIDE, 8), ROWS), :] = out[:, 128:256]
        return carry

    lax.fori_loop(0, 36, pair, 0)

    def octet(g, carry):
        out = look(lo_r[pl.ds(g, 1), :], hi_r[pl.ds(g, 1), :])
        for q in range(8):
            i = 8 * g + q
            spot = i + 4 * (i // 36)
            piece = out[:, 128 * (q // 4):128 * (q // 4) + 128]
            if q % 4:
                piece = pltpu.roll(piece, 128 - 32 * (q % 4), axis=1)
            rem[pl.ds(pl.multiple_of(spot * STRIDE, 8), ROWS), :] = piece
        return carry

    lax.fori_loop(0, 9, octet, 0)


def main_body(fields, nq, lat, left, right, comb, bm1, br1, bm0, br0, w_qkv, w_proj, w_fc1, w_fc2, out,
              xs, kk, vv, qq, ctx, rows, res):
    def put(rt, cs, block):
        n = block.shape[0]
        xs[240 * rt + 40 * cs:240 * rt + 40 * cs + n, :] = block

    put(7, 1, lat[0:160, :].astype(F32))
    put(0, 1, lat[160:320, :].astype(F32))
    for rt in range(6):
        put(rt + 1, 1, nq[rt].astype(F32))
    lhalo = left[0:320, :].astype(F32)
    rhalo = right[...].astype(F32)
    for rt in range(8):
        put(rt, 0, lhalo[40 * rt:40 * rt + 40, :])
        put(rt, 5, rhalo[40 * rt:40 * rt + 40, :])

    def project(step, carry):
        at = pl.multiple_of(step * 480, 480)
        x = xs[pl.ds(at, 480), :].astype(BF16)
        y = dot(x, w_qkv[:, C:3 * C])
        kk[pl.ds(at, 480), :] = y[:, 0:C].astype(BF16)
        vv[pl.ds(at, 480), :] = y[:, C:2 * C].astype(BF16)
        return carry

    lax.fori_loop(0, 4, project, 0)
    for rt in range(6):
        qq[rt] = dot(nq[rt], w_qkv[:, 0:C]).astype(BF16).astype(F32)

    top = lat[320:336, 0:256].astype(F32)
    lreg = left[320:336, 0:256].astype(F32)
    rows[0:4, :] = lreg[0:4, :]
    rows[4:5, :] = top[0:1, :]
    rows[8:9, :] = top[1:2, :]
    rows[5:8, :] = comb[0:3, 0:256]
    rows[9:12, :] = comb[0:3, 256:512]

    lane = lax.broadcasted_iota(jnp.int32, (1, 128), 1)
    heads = [(lane // 32 == h) for h in range(4)]
    sub = lax.broadcasted_iota(jnp.int32, (8, KEYS), 0).astype(F32)
    ones = jnp.ones((KEYS, 128), BF16)
    scale = 32 ** -0.5 * LOG2E

    def unit(r2, step, carry):
        if r2:
            t, rt = step, 2 * step + 1
            th0 = jnp.where(step == 0, 0, 4 + 12 * step)
            bm, br = bm1, br1
        else:
            t, rt = step + 1, 2 * step + 2
            th0 = jnp.where(step == 2, 0, 16 + 12 * step)
            bm, br = bm0, br0
        for w, (c0, nrow, q0) in enumerate(((40, 40, 0), (0, 80, 40), (0, 40, 120))):
            ids = rows[pl.ds(4 * w + t, 1), :][:, 0:KEYS]
            hot = jnp.where(sub == ids, 1.0, 0.0).astype(BF16)
            same = lax.dot_general(hot, hot, (((0,), (0,)), ((), ())), preferred_element_type=F32)
            same = same[80 * r2 + c0:80 * r2 + c0 + nrow, :] > 0.5
            k0 = pl.multiple_of(480 * t + 80 * w, 80)
            k1 = pl.multiple_of(480 * t + 240 + 80 * w, 80)
            q_all = qq[rt - 1, q0:q0 + nrow, :]
            for g in range(3):
                sl = slice(128 * g, 128 * g + 128)
                k = jnp.concatenate([kk[pl.ds(k0, 80), sl], kk[pl.ds(k1, 80), sl]], axis=0)
                v = jnp.concatenate([vv[pl.ds(k0, 80), sl], vv[pl.ds(k1, 80), sl]], axis=0)
                q = q_all[:, sl]
                qs = jnp.concatenate([jnp.where(m, q, 0.0) for m in heads], axis=0).astype(BF16)
                s = lax.dot_general(qs, k, (((1,), (1,)), ((), ())), preferred_element_type=F32)
                parts = []
                for h in range(4):
                    at = c0 * STRIDE + th0 + 4 * g + h
                    b = jnp.concatenate([bm[pl.ds(at, nrow, stride=STRIDE), :],
                                         br[pl.ds(at, nrow, stride=STRIDE), :][:, 0:32]], axis=1)
                    x = s[h * nrow:(h + 1) * nrow, :] * scale + b
                    x = jnp.where(same, x, -1e30)
                    x = jnp.exp2(x - jnp.max(x, axis=1, keepdims=True))
                    parts.append(x.astype(BF16))
                p = jnp.concatenate(parts, axis=0)
                o = dot(p, jnp.concatenate([v, ones], axis=1))
                c = jnp.zeros((nrow, 128), F32)
                for h in range(4):
                    oh = o[h * nrow:(h + 1) * nrow, :]
                    c = jnp.where(heads[h], oh[:, 0:128] / oh[:, 128:256], c)
                ctx[rt - 1, q0:q0 + nrow, sl] = c
        return carry

    lax.fori_loop(0, 3, lambda s, c: unit(0, s, c), 0)
    lax.fori_loop(0, 3, lambda s, c: unit(1, s, c), 0)

    def back(rt, carry):
        att = dot(ctx[rt].astype(BF16), w_proj[...]).astype(BF16).astype(F32)
        qq[rt] = att
        for level in range(2):
            for r3 in range(3):
                base = 6 * ((1 - level) * 3 + r3)
                for cs in range(4):
                    res[level * 18 + 3 * rt + r3, 6 * cs:6 * cs + 6, :] = \
                        qq[rt, 40 * cs + base:40 * cs + base + 6, :]
        return carry

    lax.fori_loop(0, 6, back, 0)

    def feed(step, carry):
        x = fields[pl.ds(9 * step, 9)].astype(F32) + res[pl.ds(9 * step, 9)]
        x = x.reshape(216, C).astype(BF16).astype(F32)
        y = dot(normalise(x), w_fc1[...])
        hidden = (0.5 * y * (1.0 + lax.erf(y * (0.5 ** 0.5)))).astype(BF16)
        z = x + dot(hidden, w_fc2[...])
        out[pl.ds(9 * step, 9)] = z.reshape(9, 24, C).astype(BF16)
        return carry

    lax.fori_loop(0, 4, feed, 0)


def call(body, outs, scratch, args, limit=48, **kw):
    return pl.pallas_call(
        body,
        out_shape=outs,
        scratch_shapes=scratch,
        compiler_params=pltpu.CompilerParams(vmem_limit_bytes=limit << 20),
        **kw,
    )(*args)


def shift(value, axis, steps):
    count = lax.axis_size(axis)
    return lax.ppermute(value, axis, [(s, (s + steps) % count) for s in range(count)])


def sds(shape, dtype):
    return jax.ShapeDtypeStruct(shape, dtype)


def local(fields, region_ids, bias_index, earth_bias, w_qkv, w_proj, w_fc1, w_fc2):
    fields = fields.reshape(36, 24, C)
    region = region_ids.reshape(36, 24)
    eb = jnp.pad(earth_bias, ((0, 0), (0, 16), (0, 0))).reshape(3, CHUNKS, 256, HEADS)
    eb = eb.transpose(1, 0, 3, 2).astype(F32)
    tab = jnp.concatenate([jnp.pad(eb[:, 2], ((0, 0), (0, 4), (0, 0))), eb[:, 0], eb[:, 1]], axis=1)
    tab = tab.reshape(CHUNKS * ROWS, 256)
    cols, keep, group, fill = region_constants()
    nq, comb, pay = call(
        prep_body,
        (sds((6, 160, C), BF16), sds((8, 512), F32), sds((544, C), BF16)),
        [pltpu.VMEM((6, 160, C), F32)],
        (fields, region, tab, jnp.asarray(cols, BF16), jnp.asarray(keep, F32), jnp.asarray(group, BF16),
         jnp.asarray(fill, F32)),
    )
    lat = shift(pay, "lat", 1)

    def bias(half, swap):
        consts = index_constants(half)
        kinds = (BF16, BF16, BF16, F32, BF16)
        return call(
            lambda *refs: bias_body(half == 0, *refs),
            (sds((80 * STRIDE, 128), F32), sds((80 * STRIDE, 128), F32)),
            [pltpu.VMEM((CHUNKS * ROWS, 256), F32), pltpu.VMEM((72, 128), F32), pltpu.VMEM((72, 128), F32),
             pltpu.VMEM((16, 256), F32), pltpu.VMEM((16, 256), F32)],
            (bias_index, tab, swap) + tuple(jnp.asarray(c, k) for c, k in zip(consts, kinds)),
            cost_estimate=pl.CostEstimate(flops=4 * 10 ** 9, transcendentals=0, bytes_accessed=4 * 10 ** 6),
        )

    bm0, br0 = bias(0, pay)
    pay_r, pay_l = call(
        lon_body,
        (sds((336, C), BF16), sds((320, C), BF16)),
        [pltpu.VMEM((320, C), F32), pltpu.VMEM((320, C), F32)],
        (nq, lat, comb),
    )
    left = shift(pay_r, "lon", 1)
    right = shift(pay_l, "lon", -1)
    bm1, br1 = bias(1, lat)
    result = call(
        main_body,
        sds((36, 24, C), BF16),
        [pltpu.VMEM((1920, C), F32), pltpu.VMEM((1920, C), BF16), pltpu.VMEM((1920, C), BF16),
         pltpu.VMEM((6, 160, C), F32), pltpu.VMEM((6, 160, C), F32), pltpu.VMEM((16, 256), F32),
         pltpu.VMEM((36, 24, C), F32)],
        (fields, nq, lat, left, right, comb, bm1, br1, bm0, br0, w_qkv, w_proj, w_fc1, w_fc2),
    )
    return result.reshape(2, 18, 24, C)


def solution(mesh):
    return jax.shard_map(
        local,
        mesh=mesh,
        in_specs=(
            P("ens", "lat", "lon", None),
            P(None, "lat", "lon"),
            P(),
            P("lat", None, None),
            P(),
            P(),
            P(),
            P(),
        ),
        out_specs=P("ens", "lat", "lon", None),
        check_vma=False,
    )
```

```python
import numpy as np
import jax
import jax.numpy as jnp
from jax import lax
from jax.experimental import pallas as pl
from jax.experimental.pallas import tpu as pltpu
from jax.sharding import PartitionSpec as P

F32 = jnp.float32
BF16 = jnp.bfloat16
EPS = 1e-05
LOG2E = 1.4426950408889634
C = 384
HEADS = 12
QUAD = 40
KEYS = 160
POSITIONS = 3312
CHUNKS = 13
ROWS = 40
SPAN = 80


def floor_div(x, d):
    return jnp.floor((x + 0.5) * (1.0 / d))


def region_constants():
    lane = lax.broadcasted_iota(jnp.int32, (1, 512), 1).astype(F32)
    w = floor_div(lane, 256)
    p = lane - 256 * w
    r2 = floor_div(p, 80)
    c2 = floor_div(p - 80 * r2, 40)
    kk = p - 80 * r2 - 40 * c2
    valid = (p < 160) & (kk < 36)
    level = floor_div(kk, 18)
    r3 = floor_div(kk - 18 * level, 6)
    src = jnp.where(valid, 12 * w + 6 * c2 + kk - 18 * level - 6 * r3, -1.0)
    lane_row = jnp.where(valid, level * 6 + r2 * 3 + r3, -1.0)
    cols = jnp.where(lax.broadcasted_iota(jnp.int32, (24, 512), 0).astype(F32) == src, 1.0, 0.0)
    row = lax.broadcasted_iota(jnp.int32, (36, 1), 0).astype(F32)
    r = floor_div(row, 2)
    row_id = (row - 2 * r) * 6 + r - 6 * floor_div(r, 6)
    keep = jnp.where(row_id == lane_row, 1.0, 0.0)
    at = floor_div(lax.broadcasted_iota(jnp.int32, (1, 36), 1).astype(F32), 12)
    group = jnp.where(lax.broadcasted_iota(jnp.int32, (8, 36), 0).astype(F32) == at, 1.0, 0.0)
    return cols.astype(BF16), keep, group.astype(BF16), jnp.where(valid, 0.0, -1.0)


def spread_table(eb, c):
    n = min(256, POSITIONS - 256 * c)
    got = eb[:, 256 * c:256 * c + n].astype(F32)
    if n < 256:
        got = jnp.concatenate([got, jnp.zeros((HEADS, 256 - n), F32)], axis=1)
    return got


def window_order(padded):
    spots = []
    for r2 in range(2):
        for c2 in range(2):
            for level in range(2):
                for r3 in range(3):
                    for c6 in range(6):
                        spots.append(level * 72 + (r2 * 3 + r3) * 12 + c2 * 6 + c6)
            if padded:
                spots += [-1] * 4
    return np.array(spots)


def index_constants():
    pick = (window_order(False)[:, None] == np.arange(144)[None]).astype(np.float32)
    place = (np.arange(144)[:, None] == window_order(True)[None]).astype(np.float32)
    tile = (np.arange(32)[:, None] == (np.arange(256) % 32)[None]).astype(np.float32)
    keep = ((np.arange(144) % 8)[:, None] == (np.arange(256) // 32)[None]).astype(np.float32)
    row = np.arange(144)
    gather = ((16 * (row // 72) + row % 72 // 8)[None] == np.arange(32)[:, None]).astype(np.float32)
    return pick, place, tile, keep, gather


def dot(a, b):
    return jnp.dot(a, b, preferred_element_type=F32)


def normalise(x):
    mean = jnp.mean(x, axis=-1, keepdims=True)
    centred = x - mean
    var = jnp.mean(centred * centred, axis=-1, keepdims=True)
    return (centred * lax.rsqrt(var + EPS)).astype(BF16)


def fetch_all(pairs, sems):
    copies = [pltpu.make_async_copy(a, b, sems.at[n]) for n, (a, b) in enumerate(pairs)]
    for copy in copies:
        copy.start()
    return copies


def prep_body(fields_hbm, region_hbm, eb_hbm, nq, comb, pay, own, xq, reg, fields, region, eb, sems):
    copies = fetch_all(((fields_hbm, fields), (region_hbm, region), (eb_hbm.at[2], eb)), sems)
    for cs in range(4):
        for rt in range(6):
            xq[rt, 40 * cs + 32:40 * cs + 40, :] = jnp.zeros((8, C), F32)

    copies[0].wait()

    def triple(rt, carry):
        for level in range(2):
            for r3 in range(3):
                x = fields[level * 18 + 3 * rt + r3].astype(F32)
                n = normalise(x).astype(F32)
                base = 6 * ((1 - level) * 3 + r3)
                for cs in range(4):
                    xq[rt, 40 * cs + base:40 * cs + base + 6, :] = n[6 * cs:6 * cs + 6, :]
        return carry

    lax.fori_loop(0, 6, triple, 0)
    copies[1].wait()
    for r in range(18):
        reg[2 * r:2 * r + 2, :] = region[r].astype(F32)
    cols, keep, group, fill = region_constants()
    spread = dot(reg[...].astype(BF16), cols) * keep
    rows = dot(group, spread.astype(BF16)) + fill
    comb[...] = rows
    nq[...] = xq[...].astype(BF16)
    pay[0:160, :] = xq[0].astype(BF16)
    pay[160:320, :] = xq[5].astype(BF16)
    last = jnp.concatenate([rows[2:3, 0:256], rows[2:3, 256:512], jnp.zeros((14, 256), F32)], axis=0)
    pay[320:336, 0:256] = last.astype(BF16)
    copies[2].wait()
    for c in range(CHUNKS):
        own[c] = jnp.concatenate([spread_table(eb, c), jnp.zeros((4, 256), F32)], axis=0)
        pay[336 + 16 * c:352 + 16 * c, 0:256] = own[c].astype(BF16)


def lon_body(nq, lat, comb, pay_r, pay_l, scr_r, scr_l):
    first = lat[160:320, :].astype(F32)
    final = lat[0:160, :].astype(F32)
    scr_r[0:40, :] = first[120:160, :]
    scr_l[0:40, :] = first[0:40, :]
    scr_r[280:320, :] = final[120:160, :]
    scr_l[280:320, :] = final[0:40, :]
    for rt in range(6):
        own = nq[rt].astype(F32)
        scr_r[40 * rt + 40:40 * rt + 80, :] = own[120:160, :]
        scr_l[40 * rt + 40:40 * rt + 80, :] = own[0:40, :]
    pay_r[0:320, :] = scr_r[...].astype(BF16)
    pay_l[...] = scr_l[...].astype(BF16)
    top = lat[320:336, 0:256].astype(F32)
    rows = jnp.concatenate([top[1:2, :], comb[0:3, 256:512], jnp.zeros((12, 256), F32)], axis=0)
    pay_r[320:336, 0:256] = rows.astype(BF16)


def index_body(index_hbm, eb_hbm, *refs):
    consts, (lo_m, hi_m, lo_r, hi_r, inner, index, eb), bufs, sems = refs[:5], refs[5:12], refs[12:17], refs[17]
    copies = fetch_all(((index_hbm, index),) + tuple(zip(consts, bufs)) + ((eb_hbm.at[0:2], eb),), sems)
    for copy in copies[:6]:
        copy.wait()
    pick, place, tile, keep, gather = bufs
    idx = index[...]
    for part, m_ref, r_ref in ((idx & 255, lo_m, lo_r), (idx >> 8, hi_m, hi_r)):
        picked = dot(pick[...], part.astype(F32).astype(BF16)).astype(BF16)
        full = dot(picked, place[...])
        m_ref[...] = full[:, 0:128]
        wide = dot(full[:, 128:160].astype(BF16), tile[...]) * keep[...]
        r_ref[...] = dot(gather[...], wide.astype(BF16))
    copies[6].wait()
    for c in range(CHUNKS):
        inner[c, 0:12, :] = spread_table(eb.at[0], c)
        inner[c, 12:24, :] = spread_table(eb.at[1], c)


def bias_body(lo_m, hi_m, lo_r, hi_r, own, inner, swap, main0, rem0, main1, rem1, tabs):
    low = lax.broadcasted_iota(jnp.int32, (256, 256), 0).astype(F32)

    def look(table, lo, hi):
        hot = jnp.where(low == lo, 1.0, 0.0).astype(BF16)
        got = dot(table, hot)
        out = got[0:ROWS]
        for c in range(1, CHUNKS):
            out = jnp.where(hi == float(c), got[ROWS * c:ROWS * c + ROWS], out)
        return out * LOG2E

    for c in range(CHUNKS):
        tabs[ROWS * c + 16:ROWS * c + ROWS, :] = inner[c]

    for half, main, rem in ((0, main0, rem0), (1, main1, rem1)):
        for c in range(CHUNKS):
            tabs[ROWS * c:ROWS * c + 16, :] = \
                swap[336 + 16 * c:352 + 16 * c, 0:256].astype(F32) if half else own[c]
        table = tabs[...].astype(BF16)

        def pair(step, carry):
            i = 2 * step
            at = 72 * half + i
            lo = jnp.concatenate([lo_m[pl.ds(at, 1), :], lo_m[pl.ds(at + 1, 1), :]], axis=1)
            hi = jnp.concatenate([hi_m[pl.ds(at, 1), :], hi_m[pl.ds(at + 1, 1), :]], axis=1)
            out = look(table, lo, hi)
            spot = i + 4 * (i // 36)
            main[pl.ds(spot, ROWS, stride=SPAN), :] = out[:, 0:128]
            main[pl.ds(spot + 1, ROWS, stride=SPAN), :] = out[:, 128:256]
            return carry

        lax.fori_loop(0, 36, pair, 0, unroll=12)

        def octet(g, carry):
            out = look(table, lo_r[pl.ds(16 * half + g, 1), :], hi_r[pl.ds(16 * half + g, 1), :])
            for q in range(8):
                i = 8 * g + q
                spot = i + 4 * (i // 36)
                piece = out[:, 128 * (q // 4):128 * (q // 4) + 128]
                if q % 4:
                    piece = pltpu.roll(piece, 128 - 32 * (q % 4), axis=1)
                rem[pl.ds(spot, ROWS, stride=SPAN), :] = piece
            return carry

        lax.fori_loop(0, 9, octet, 0, unroll=9)


def main_body(fields, nq, lat, left, right, comb, bm1, br1, bm0, br0, w_qkv, w_proj, w_fc1, w_fc2, out,
              xs, kk, vv, qq, ctx, rows, res, qf, kf, sc, mx):
    def put(rt, cs, block):
        n = block.shape[0]
        xs[240 * rt + 40 * cs:240 * rt + 40 * cs + n, :] = block

    put(7, 1, lat[0:160, :].astype(F32))
    put(0, 1, lat[160:320, :].astype(F32))
    for rt in range(6):
        put(rt + 1, 1, nq[rt].astype(F32))
    lhalo = left[0:320, :].astype(F32)
    rhalo = right[...].astype(F32)
    for rt in range(8):
        put(rt, 0, lhalo[40 * rt:40 * rt + 40, :])
        put(rt, 5, rhalo[40 * rt:40 * rt + 40, :])

    def project(step, carry):
        at = pl.multiple_of(step * 480, 480)
        x = xs[pl.ds(at, 480), :].astype(BF16)
        y = dot(x, w_qkv[:, C:3 * C])
        kk[pl.ds(at, 480), :] = y[:, 0:C].astype(BF16)
        vv[pl.ds(at, 480), :] = y[:, C:2 * C].astype(BF16)
        return carry

    lax.fori_loop(0, 4, project, 0, unroll=4)
    for rt in range(6):
        qq[rt] = dot(nq[rt], w_qkv[:, 0:C]).astype(BF16).astype(F32)

    top = lat[320:336, 0:256].astype(F32)
    lreg = left[320:336, 0:256].astype(F32)
    rows[0:4, :] = lreg[0:4, :]
    rows[4:5, :] = top[0:1, :]
    rows[8:9, :] = top[1:2, :]
    rows[5:8, :] = comb[0:3, 0:256]
    rows[9:12, :] = comb[0:3, 256:512]

    lane = lax.broadcasted_iota(jnp.int32, (1, 128), 1)
    heads = [(lane // 32 == h) for h in range(4)]
    rows[12:16, :] = jnp.full((4, 256), -1.0, F32)
    sub = lax.broadcasted_iota(jnp.int32, (8, KEYS), 0).astype(F32)
    hot = jnp.concatenate([jnp.where(sub == rows[n:n + 1, 0:KEYS], 1.0, 0.0) for n in range(16)], axis=0)
    eye = lax.broadcasted_iota(jnp.int32, (128, 128), 0) == lax.broadcasted_iota(jnp.int32, (128, 128), 1)
    seen = lax.dot_general(hot.astype(BF16), jnp.where(eye, 1.0, 0.0).astype(BF16), (((0,), (0,)), ((), ())),
                           preferred_element_type=F32)
    qf[...] = seen
    kf[...] = (seen - 1.0) * 1e30
    ones = jnp.ones((KEYS, 128), BF16)
    scale = 32 ** -0.5 * LOG2E
    spans = ((40, 40, 0), (0, 80, 40), (0, 40, 120))

    def places(r2, step):
        return (step, 2 * step + 1) if r2 else (step + 1, 2 * step + 2)

    def window(ref, t, w, sl):
        k0 = pl.multiple_of(480 * t + 80 * w, 80)
        k1 = pl.multiple_of(480 * t + 240 + 80 * w, 80)
        return jnp.concatenate([ref[pl.ds(k0, 80), sl], ref[pl.ds(k1, 80), sl]], axis=0)

    def score(r2, step):
        t, rt = places(r2, step)
        if r2:
            th0 = jnp.where(step == 0, 0, 4 + 12 * step)
            bm, br = bm1, br1
        else:
            th0 = jnp.where(step == 2, 0, 16 + 12 * step)
            bm, br = bm0, br0
        for w, (c0, nrow, q0) in enumerate(spans):
            far = jnp.where(lane // 8 == 4 * w + t, kf[...], 0.0).astype(BF16)
            near = qf[80 * r2 + c0:80 * r2 + c0 + nrow, :]
            for g in range(3):
                sl = slice(128 * g, 128 * g + 128)
                k = jnp.concatenate([window(kk, t, w, sl), far], axis=1)
                q = qq[rt - 1, q0:q0 + nrow, sl]
                qs = jnp.concatenate([jnp.concatenate([jnp.where(m, q, 0.0), near], axis=1) for m in heads],
                                     axis=0).astype(BF16)
                at = 640 * g + 4 * q0
                s = lax.dot_general(qs, k, (((1,), (1,)), ((), ())), preferred_element_type=F32)
                for h in range(4):
                    th = pl.multiple_of((th0 + 4 * g + h) * SPAN, SPAN) + c0
                    b = jnp.concatenate([bm[pl.ds(th, nrow), :], br[pl.ds(th, nrow), :][:, 0:32]], axis=1)
                    x = s[h * nrow:(h + 1) * nrow, :] * scale + b
                    sc[r2, at + h * nrow:at + (h + 1) * nrow, :] = x
                    mx[r2, at + h * nrow:at + (h + 1) * nrow, :] = jnp.broadcast_to(
                        jnp.max(x, axis=1, keepdims=True), (nrow, 128))

    def attend(r2, step):
        t, rt = places(r2, step)
        for w, (c0, nrow, q0) in enumerate(spans):
            for g in range(3):
                sl = slice(128 * g, 128 * g + 128)
                at = 640 * g + 4 * q0
                parts = []
                for h in range(4):
                    x = sc[r2, at + h * nrow:at + (h + 1) * nrow, :]
                    m = mx[r2, at + h * nrow:at + (h + 1) * nrow, :]
                    x = x - jnp.concatenate([m, m[:, 0:32]], axis=1)
                    parts.append(jnp.exp2(x).astype(BF16))
                o = dot(jnp.concatenate(parts, axis=0), jnp.concatenate([window(vv, t, w, sl), ones], axis=1))
                os = [o[h * nrow:(h + 1) * nrow, :] for h in range(4)]
                num, den = os[3][:, 0:128], os[3][:, 128:256]
                for h in range(3):
                    num = jnp.where(heads[h], os[h][:, 0:128], num)
                    den = jnp.where(heads[h], os[h][:, 128:256], den)
                ctx[rt - 1, q0:q0 + nrow, sl] = num / den

    score(0, 0)

    def steps(step, carry):
        score(1, step)
        attend(0, step)
        score(0, jnp.minimum(step + 1, 2))
        attend(1, step)
        return carry

    lax.fori_loop(0, 3, steps, 0)

    def back(rt, carry):
        att = dot(ctx[rt].astype(BF16), w_proj[...]).astype(BF16).astype(F32)
        qq[rt] = att
        for level in range(2):
            for r3 in range(3):
                base = 6 * ((1 - level) * 3 + r3)
                for cs in range(4):
                    res[level * 18 + 3 * rt + r3, 6 * cs:6 * cs + 6, :] = \
                        qq[rt, 40 * cs + base:40 * cs + base + 6, :]
        return carry

    lax.fori_loop(0, 6, back, 0, unroll=6)

    def feed(step, carry):
        x = fields[pl.ds(9 * step, 9)].astype(F32) + res[pl.ds(9 * step, 9)]
        x = x.reshape(216, C).astype(BF16).astype(F32)
        y = dot(normalise(x), w_fc1[...])
        hidden = (0.5 * y * (1.0 + lax.erf(y * (0.5 ** 0.5)))).astype(BF16)
        z = x + dot(hidden, w_fc2[...])
        out[pl.ds(9 * step, 9)] = z.reshape(9, 24, C).astype(BF16)
        return carry

    lax.fori_loop(0, 4, feed, 0, unroll=4)


def call(body, outs, scratch, args, limit=28, **kw):
    return pl.pallas_call(
        body,
        out_shape=outs,
        scratch_shapes=scratch,
        compiler_params=pltpu.CompilerParams(vmem_limit_bytes=limit << 20),
        **kw,
    )(*args)


def hold(x):
    return pltpu.with_memory_space_constraint(x, pltpu.HBM)


def shift(value, axis, steps):
    count = lax.axis_size(axis)
    return lax.ppermute(value, axis, [(s, (s + steps) % count) for s in range(count)])


def sds(shape, dtype):
    return jax.ShapeDtypeStruct(shape, dtype)


def local(fields, region_ids, bias_index, earth_bias, w_qkv, w_proj, w_fc1, w_fc2):
    fields = fields.reshape(36, 24, C)
    region = region_ids.transpose(1, 0, 2)
    tables = earth_bias.transpose(0, 2, 1)
    nq, comb, pay, own = call(
        prep_body,
        (sds((6, 160, C), BF16), sds((8, 512), F32), sds((544, C), BF16), sds((CHUNKS, 16, 256), F32)),
        [pltpu.VMEM((6, 160, C), F32), pltpu.VMEM((36, 24), F32), pltpu.VMEM((36, 24, C), BF16),
         pltpu.VMEM((18, 2, 24), jnp.int32), pltpu.VMEM((HEADS, POSITIONS), BF16), pltpu.SemaphoreType.DMA((3,))],
        tuple(hold(x) for x in (fields, region, tables)),
        in_specs=[pl.BlockSpec(memory_space=pltpu.HBM)] * 3,
    )
    lat = shift(pay, "lat", 1)

    kinds = (BF16, BF16, BF16, F32, BF16)
    consts = tuple(jnp.asarray(c, k) for c, k in zip(index_constants(), kinds))
    *found, inner = call(
        index_body,
        (sds((144, 128), F32), sds((144, 128), F32), sds((32, 256), F32), sds((32, 256), F32),
         sds((CHUNKS, 24, 256), F32)),
        [pltpu.VMEM((144, 144), jnp.int32), pltpu.VMEM((2, HEADS, POSITIONS), BF16)] +
        [pltpu.VMEM(c.shape, c.dtype) for c in consts] + [pltpu.SemaphoreType.DMA((7,))],
        tuple(hold(x) for x in (bias_index, tables) + consts),
        in_specs=[pl.BlockSpec(memory_space=pltpu.HBM)] * 7,
        cost_estimate=pl.CostEstimate(flops=10 ** 9, transcendentals=0, bytes_accessed=10 ** 6),
    )
    pay_r, pay_l = call(
        lon_body,
        (sds((336, C), BF16), sds((320, C), BF16)),
        [pltpu.VMEM((320, C), F32), pltpu.VMEM((320, C), F32)],
        (nq, lat, comb),
    )
    left = shift(pay_r, "lon", 1)
    right = shift(pay_l, "lon", -1)
    bm0, br0, bm1, br1 = call(
        bias_body,
        (sds((ROWS * SPAN, 128), F32),) * 4,
        [pltpu.VMEM((CHUNKS * ROWS, 256), F32)],
        tuple(found) + (own, inner, lat),
        cost_estimate=pl.CostEstimate(flops=10 ** 10, transcendentals=0, bytes_accessed=8 * 10 ** 6),
    )
    result = call(
        main_body,
        sds((36, 24, C), BF16),
        [pltpu.VMEM((1920, C), F32), pltpu.VMEM((1920, C), BF16), pltpu.VMEM((1920, C), BF16),
         pltpu.VMEM((6, 160, C), F32), pltpu.VMEM((6, 160, C), F32), pltpu.VMEM((16, 256), F32),
         pltpu.VMEM((36, 24, C), F32), pltpu.VMEM((KEYS, 128), F32), pltpu.VMEM((KEYS, 128), F32),
         pltpu.VMEM((2, 1920, KEYS), F32),
         pltpu.VMEM((2, 1920, 128), F32)],
        (fields, nq, lat, left, right, comb, bm1, br1, bm0, br0, w_qkv, w_proj, w_fc1, w_fc2),
    )
    return result.reshape(2, 18, 24, C)


def solution(mesh):
    return jax.shard_map(
        local,
        mesh=mesh,
        in_specs=(
            P("ens", "lat", "lon", None),
            P(None, "lat", "lon"),
            P(),
            P("lat", None, None),
            P(),
            P(),
            P(),
            P(),
        ),
        out_specs=P("ens", "lat", "lon", None),
        check_vma=False,
    )
```

```python
import numpy as np
import jax
import jax.numpy as jnp
from jax import lax
from jax.experimental import pallas as pl
from jax.experimental.pallas import tpu as pltpu
from jax.sharding import PartitionSpec as P

F32 = jnp.float32
BF16 = jnp.bfloat16
EPS = 1e-05
LOG2E = 1.4426950408889634
C = 384
HEADS = 12
KEYS = 160
POSITIONS = 3312
CHUNKS = 13
ROWS = 40
SPAN = 80


def floor_div(x, d):
    return jnp.floor((x + 0.5) * (1.0 / d))


def region_constants():
    lane = lax.broadcasted_iota(jnp.int32, (1, 512), 1).astype(F32)
    w = floor_div(lane, 256)
    p = lane - 256 * w
    r2 = floor_div(p, 80)
    c2 = floor_div(p - 80 * r2, 40)
    kk = p - 80 * r2 - 40 * c2
    valid = (p < 160) & (kk < 36)
    level = floor_div(kk, 18)
    r3 = floor_div(kk - 18 * level, 6)
    src = jnp.where(valid, 12 * w + 6 * c2 + kk - 18 * level - 6 * r3, -1.0)
    lane_row = jnp.where(valid, level * 6 + r2 * 3 + r3, -1.0)
    cols = jnp.where(lax.broadcasted_iota(jnp.int32, (24, 512), 0).astype(F32) == src, 1.0, 0.0)
    row = lax.broadcasted_iota(jnp.int32, (36, 1), 0).astype(F32)
    r = floor_div(row, 2)
    row_id = (row - 2 * r) * 6 + r - 6 * floor_div(r, 6)
    keep = jnp.where(row_id == lane_row, 1.0, 0.0)
    at = floor_div(lax.broadcasted_iota(jnp.int32, (1, 36), 1).astype(F32), 12)
    group = jnp.where(lax.broadcasted_iota(jnp.int32, (8, 36), 0).astype(F32) == at, 1.0, 0.0)
    return cols.astype(BF16), keep, group.astype(BF16), jnp.where(valid, 0.0, -1.0)


def spread_table(eb, c):
    n = min(256, POSITIONS - 256 * c)
    got = eb[:, 256 * c:256 * c + n].astype(F32)
    if n < 256:
        got = jnp.concatenate([got, jnp.zeros((HEADS, 256 - n), F32)], axis=1)
    return got


def window_order(padded):
    spots = []
    for r2 in range(2):
        for c2 in range(2):
            for level in range(2):
                for r3 in range(3):
                    for c6 in range(6):
                        spots.append(level * 72 + (r2 * 3 + r3) * 12 + c2 * 6 + c6)
            if padded:
                spots += [-1] * 4
    return np.array(spots)


def index_constants():
    pick = (window_order(False)[:, None] == np.arange(144)[None]).astype(np.float32)
    place = (np.arange(144)[:, None] == window_order(True)[None]).astype(np.float32)
    tile = (np.arange(32)[:, None] == (np.arange(256) % 32)[None]).astype(np.float32)
    keep = ((np.arange(144) % 8)[:, None] == (np.arange(256) // 32)[None]).astype(np.float32)
    row = np.arange(144)
    gather = ((16 * (row // 72) + row % 72 // 8)[None] == np.arange(32)[:, None]).astype(np.float32)
    return pick, place, tile, keep, gather


def dot(a, b):
    return jnp.dot(a, b, preferred_element_type=F32)


def normalise(x):
    mean = jnp.mean(x, axis=-1, keepdims=True)
    centred = x - mean
    var = jnp.mean(centred * centred, axis=-1, keepdims=True)
    return (centred * lax.rsqrt(var + EPS)).astype(BF16)


def fetch_all(pairs, sems):
    copies = [pltpu.make_async_copy(a, b, sems.at[n]) for n, (a, b) in enumerate(pairs)]
    for copy in copies:
        copy.start()
    return copies


def prep_body(fields_hbm, region_hbm, eb_hbm, nq, comb, pay, own, xq, reg, fields, region, eb, sems):
    copies = fetch_all(((fields_hbm, fields), (region_hbm, region), (eb_hbm.at[2], eb)), sems)
    for cs in range(4):
        for rt in range(6):
            xq[rt, 40 * cs + 32:40 * cs + 40, :] = jnp.zeros((8, C), F32)

    copies[0].wait()

    def triple(rt, carry):
        for level in range(2):
            for r3 in range(3):
                x = fields[level * 18 + 3 * rt + r3].astype(F32)
                n = normalise(x).astype(F32)
                base = 6 * ((1 - level) * 3 + r3)
                for cs in range(4):
                    xq[rt, 40 * cs + base:40 * cs + base + 6, :] = n[6 * cs:6 * cs + 6, :]
        return carry

    lax.fori_loop(0, 6, triple, 0, unroll=3)
    copies[1].wait()
    for r in range(18):
        reg[2 * r:2 * r + 2, :] = region[r].astype(F32)
    cols, keep, group, fill = region_constants()
    spread = dot(reg[...].astype(BF16), cols) * keep
    rows = dot(group, spread.astype(BF16)) + fill
    comb[...] = rows
    nq[...] = xq[...].astype(BF16)
    pay[0:160, :] = xq[0].astype(BF16)
    pay[160:320, :] = xq[5].astype(BF16)
    last = jnp.concatenate([rows[2:3, 0:256], rows[2:3, 256:512], jnp.zeros((14, 256), F32)], axis=0)
    pay[320:336, 0:256] = last.astype(BF16)
    copies[2].wait()
    for c in range(CHUNKS):
        own[c] = jnp.concatenate([spread_table(eb, c), jnp.zeros((4, 256), F32)], axis=0)
        pay[336 + 16 * c:352 + 16 * c, 0:256] = own[c].astype(BF16)


def column(nq, lat, scr, cs):
    sl = slice(40 * cs, 40 * cs + 40)
    scr[0:40, :] = lat[160:320, :].astype(F32)[sl, :]
    scr[280:320, :] = lat[0:160, :].astype(F32)[sl, :]
    for rt in range(6):
        scr[40 * rt + 40:40 * rt + 80, :] = nq[rt].astype(F32)[sl, :]
    return scr[...].astype(BF16)


def right_body(nq, lat, comb, pay, scr):
    pay[0:320, :] = column(nq, lat, scr, 3)
    top = lat[320:336, 0:256].astype(F32)
    rows = jnp.concatenate([top[1:2, :], comb[0:3, 256:512], jnp.zeros((12, 256), F32)], axis=0)
    pay[320:336, 0:256] = rows.astype(BF16)


def left_body(nq, lat, after, pay, scr):
    pay[...] = column(nq, lat, scr, 0)


def index_body(index_hbm, eb_hbm, *refs):
    consts, (lo_m, hi_m, lo_r, hi_r, inner, index, eb), bufs, sems = refs[:5], refs[5:12], refs[12:17], refs[17]
    copies = fetch_all(((index_hbm, index),) + tuple(zip(consts, bufs)) + ((eb_hbm.at[0:2], eb),), sems)
    for copy in copies[:6]:
        copy.wait()
    pick, place, tile, keep, gather = bufs
    idx = index[...]
    for part, m_ref, r_ref in ((idx & 255, lo_m, lo_r), (idx >> 8, hi_m, hi_r)):
        picked = dot(pick[...], part.astype(F32).astype(BF16)).astype(BF16)
        full = dot(picked, place[...])
        m_ref[...] = full[:, 0:128]
        wide = dot(full[:, 128:160].astype(BF16), tile[...]) * keep[...]
        r_ref[...] = dot(gather[...], wide.astype(BF16))
    copies[6].wait()
    for c in range(CHUNKS):
        inner[c, 0:12, :] = spread_table(eb.at[0], c)
        inner[c, 12:24, :] = spread_table(eb.at[1], c)


def early_blocks():
    return jnp.maximum(7 - lax.axis_index("lon") % 32, 0)


def bias_body(late, lo_m, hi_m, lo_r, hi_r, own, inner, swap, *refs):
    main0, rem0, main1, rem1, tabs = refs[4:] if late else refs
    low = lax.broadcasted_iota(jnp.int32, (256, 256), 0).astype(F32)
    early = early_blocks()

    def look(table, lo, hi):
        hot = jnp.where(low == lo, 1.0, 0.0).astype(BF16)
        got = dot(table, hot)
        out = got[0:ROWS]
        for c in range(1, CHUNKS):
            out = jnp.where(hi == float(c), got[ROWS * c:ROWS * c + ROWS], out)
        return out * LOG2E

    for c in range(CHUNKS):
        tabs[ROWS * c + 16:ROWS * c + ROWS, :] = inner[c]

    for half, main, rem in ((0, main0, rem0), (1, main1, rem1)):
        for c in range(CHUNKS):
            tabs[ROWS * c:ROWS * c + 16, :] = \
                swap[336 + 16 * c:352 + 16 * c, 0:256].astype(F32) if half else own[c]
        table = tabs[...].astype(BF16)
        done = jnp.clip(early - 4 * half, 0, 4)

        def pairs(block, carry):
            first = 24 * block
            for step in range(12):
                at = 72 * half + first + 2 * step
                lo = jnp.concatenate([lo_m[pl.ds(at, 1), :], lo_m[pl.ds(at + 1, 1), :]], axis=1)
                hi = jnp.concatenate([hi_m[pl.ds(at, 1), :], hi_m[pl.ds(at + 1, 1), :]], axis=1)
                out = look(table, lo, hi)
                spot = first + 2 * step
                spot = spot + jnp.where(spot >= 36, 4, 0)
                main[pl.ds(spot, ROWS, stride=SPAN), :] = out[:, 0:128]
                main[pl.ds(spot + 1, ROWS, stride=SPAN), :] = out[:, 128:256]
            return carry

        if late:
            lax.fori_loop(jnp.minimum(done, 3), 3, pairs, 0)
        else:
            lax.fori_loop(0, jnp.minimum(done, 3), pairs, 0)

        @pl.when(done < 4 if late else done >= 4)
        def _():
            for g in range(9):
                out = look(table, lo_r[16 * half + g:16 * half + g + 1, :], hi_r[16 * half + g:16 * half + g + 1, :])
                for q in range(8):
                    i = 8 * g + q
                    spot = i + 4 * (i // 36)
                    piece = out[:, 128 * (q // 4):128 * (q // 4) + 128]
                    if q % 4:
                        piece = pltpu.roll(piece, 128 - 32 * (q % 4), axis=1)
                    rem[pl.ds(spot, ROWS, stride=SPAN), :] = piece


SPANS = ((40, 40, 0), (0, 80, 40), (0, 40, 120))
SCALE = 32 ** -0.5 * LOG2E


def head_lanes():
    lane = lax.broadcasted_iota(jnp.int32, (1, 128), 1)
    return lane, [(lane // 32 == h) for h in range(4)]


def put(xs, group, rt, second, block):
    at = 640 * group + 80 * rt + 40 * second
    xs[at:at + block.shape[0], :] = block


def key_values(xs, kk, vv, w_qkv, count):
    def project(step, carry):
        at = pl.multiple_of(step * 320, 320)
        y = dot(xs[pl.ds(at, 320), :].astype(BF16), w_qkv[:, C:3 * C])
        kk[pl.ds(at, 320), :] = y[:, 0:C].astype(BF16)
        vv[pl.ds(at, 320), :] = y[:, C:2 * C].astype(BF16)
        return carry

    lax.fori_loop(0, count, project, 0, unroll=count)


def region_features(rows, qf, kf):
    sub = lax.broadcasted_iota(jnp.int32, (8, KEYS), 0).astype(F32)
    hot = jnp.concatenate([jnp.where(sub == rows[n:n + 1, 0:KEYS], 1.0, 0.0) for n in range(8)], axis=0)
    eye = lax.broadcasted_iota(jnp.int32, (64, 128), 0) == lax.broadcasted_iota(jnp.int32, (64, 128), 1)
    seen = lax.dot_general(
        jnp.concatenate([hot, jnp.zeros((64, KEYS), F32)], axis=0).astype(BF16),
        jnp.concatenate([jnp.where(eye, 1.0, 0.0), jnp.zeros((64, 128), F32)], axis=0).astype(BF16),
        (((0,), (0,)), ((), ())), preferred_element_type=F32)
    qf[...] = seen
    kf[...] = (seen - 1.0) * 1e30


def attention(windows, tables, qq, kk, vv, qf, kf, sc, mx, store):
    lane, heads = head_lanes()
    ones = jnp.ones((KEYS, 128), BF16)

    def places(r2, step):
        return (step, 2 * step + 1) if r2 else (step + 1, 2 * step + 2)

    def score(r2, step):
        t, rt = places(r2, step)
        if r2:
            th0 = jnp.where(step == 0, 0, 4 + 12 * step)
        else:
            th0 = jnp.where(step == 2, 0, 16 + 12 * step)
        bm, br = tables[r2]
        top = 0
        for n, w in enumerate(windows):
            c0, nrow, q0 = SPANS[w]
            far = jnp.where(lane // 8 == 4 * n + t, kf[...], 0.0).astype(BF16)
            near = qf[80 * r2 + c0:80 * r2 + c0 + nrow, :]
            for g in range(3):
                sl = slice(128 * g, 128 * g + 128)
                k = jnp.concatenate([kk[pl.ds(pl.multiple_of(640 * n + 160 * t, 160), KEYS), sl], far], axis=1)
                q = qq[rt - 1, q0:q0 + nrow, sl]
                qs = jnp.concatenate([jnp.concatenate([jnp.where(m, q, 0.0), near], axis=1) for m in heads],
                                     axis=0).astype(BF16)
                s = lax.dot_general(qs, k, (((1,), (1,)), ((), ())), preferred_element_type=F32)
                for h in range(4):
                    th = pl.multiple_of((th0 + 4 * g + h) * SPAN, SPAN) + c0
                    b = jnp.concatenate([bm[pl.ds(th, nrow), :], br[pl.ds(th, nrow), :][:, 0:32]], axis=1)
                    x = s[h * nrow:(h + 1) * nrow, :] * SCALE + b
                    sc[r2, top:top + nrow, :] = x
                    mx[r2, top:top + nrow, :] = jnp.broadcast_to(jnp.max(x, axis=1, keepdims=True), (nrow, 128))
                    top += nrow

    def attend(r2, step):
        t, rt = places(r2, step)
        top = 0
        for n, w in enumerate(windows):
            _, nrow, _ = SPANS[w]
            for g in range(3):
                sl = slice(128 * g, 128 * g + 128)
                parts = []
                for _ in range(4):
                    m = mx[r2, top:top + nrow, :]
                    x = sc[r2, top:top + nrow, :] - jnp.concatenate([m, m[:, 0:32]], axis=1)
                    parts.append(jnp.exp2(x).astype(BF16))
                    top += nrow
                v = vv[pl.ds(pl.multiple_of(640 * n + 160 * t, 160), KEYS), sl]
                o = dot(jnp.concatenate(parts, axis=0), jnp.concatenate([v, ones], axis=1))
                os = [o[h * nrow:(h + 1) * nrow, :] for h in range(4)]
                num, den = os[3][:, 0:128], os[3][:, 128:256]
                for h in range(3):
                    num = jnp.where(heads[h], os[h][:, 0:128], num)
                    den = jnp.where(heads[h], os[h][:, 128:256], den)
                store(rt - 1, w, sl, num / den)

    score(0, 0)

    def steps(step, carry):
        score(1, step)
        attend(0, step)
        score(0, jnp.minimum(step + 1, 2))
        attend(1, step)
        return carry

    lax.fori_loop(0, 3, steps, 0)


def inner_body(nq, lat, comb, bm1, br1, bm0, br0, w_qkv, qq, ctx, xs, kk, vv, rows, qf, kf, sc, mx):
    xs[0:80, :] = lat[200:280, :].astype(F32)
    xs[560:640, :] = lat[0:160, :].astype(F32)[40:120, :]
    for rt in range(6):
        xs[80 * rt + 80:80 * rt + 160, :] = nq[rt].astype(F32)[40:120, :]
    key_values(xs, kk, vv, w_qkv, 2)
    for rt in range(6):
        qq[rt] = dot(nq[rt], w_qkv[:, 0:C]).astype(BF16).astype(F32)
    rows[...] = jnp.full((8, 256), -1.0, F32)
    rows[0:1, :] = lat[320:336, 0:256].astype(F32)[0:1, :]
    rows[1:4, :] = comb[0:3, 0:256]
    region_features(rows, qf, kf)

    def store(rt, w, sl, value):
        ctx[rt, :, sl] = value

    attention((1,), ((bm0, br0), (bm1, br1)), qq, kk, vv, qf, kf, sc, mx, store)


def outer_body(fields, nq, lat, left, right, comb, qq, mid, bm1, br1, bm0, br0, w_qkv, w_proj, w_fc1, w_fc2, out,
               xs, kk, vv, ctx, att, rows, res, qf, kf, sc, mx):
    below = lat[0:160, :].astype(F32)
    above = lat[160:320, :].astype(F32)
    put(xs, 0, 0, 1, above[0:40, :])
    put(xs, 1, 0, 0, above[120:160, :])
    put(xs, 0, 7, 1, below[0:40, :])
    put(xs, 1, 7, 0, below[120:160, :])
    lhalo = left[0:320, :].astype(F32)
    rhalo = right[...].astype(F32)
    for rt in range(8):
        put(xs, 0, rt, 0, lhalo[40 * rt:40 * rt + 40, :])
        put(xs, 1, rt, 1, rhalo[40 * rt:40 * rt + 40, :])
    for rt in range(6):
        own = nq[rt].astype(F32)
        put(xs, 0, rt + 1, 1, own[0:40, :])
        put(xs, 1, rt + 1, 0, own[120:160, :])
        ctx[rt, 40:120, :] = mid[rt]
    key_values(xs, kk, vv, w_qkv, 4)
    rows[0:4, :] = left[320:336, 0:256].astype(F32)[0:4, :]
    rows[4:5, :] = lat[320:336, 0:256].astype(F32)[1:2, :]
    rows[5:8, :] = comb[0:3, 256:512]
    region_features(rows, qf, kf)

    def store(rt, w, sl, value):
        ctx[rt, SPANS[w][2]:SPANS[w][2] + 40, sl] = value

    attention((0, 2), ((bm0, br0), (bm1, br1)), qq, kk, vv, qf, kf, sc, mx, store)

    def back(rt, carry):
        att[rt] = dot(ctx[rt].astype(BF16), w_proj[...]).astype(BF16).astype(F32)
        for level in range(2):
            for r3 in range(3):
                base = 6 * ((1 - level) * 3 + r3)
                for cs in range(4):
                    res[level * 18 + 3 * rt + r3, 6 * cs:6 * cs + 6, :] = \
                        att[rt, 40 * cs + base:40 * cs + base + 6, :]
        return carry

    lax.fori_loop(0, 6, back, 0, unroll=6)

    def feed(step, carry):
        x = fields[pl.ds(9 * step, 9)].astype(F32) + res[pl.ds(9 * step, 9)]
        x = x.reshape(216, C).astype(BF16).astype(F32)
        y = dot(normalise(x), w_fc1[...])
        hidden = (0.5 * y * (1.0 + lax.erf(y * (0.5 ** 0.5)))).astype(BF16)
        z = x + dot(hidden, w_fc2[...])
        out[pl.ds(9 * step, 9)] = z.reshape(9, 24, C).astype(BF16)
        return carry

    lax.fori_loop(0, 4, feed, 0, unroll=4)


def call(body, outs, scratch, args, limit=28, **kw):
    return pl.pallas_call(
        body,
        out_shape=outs,
        scratch_shapes=scratch,
        compiler_params=pltpu.CompilerParams(vmem_limit_bytes=limit << 20),
        **kw,
    )(*args)


def hold(x):
    return pltpu.with_memory_space_constraint(x, pltpu.HBM)


def shift(value, axis, steps):
    count = lax.axis_size(axis)
    return lax.ppermute(value, axis, [(s, (s + steps) % count) for s in range(count)])


def sds(shape, dtype):
    return jax.ShapeDtypeStruct(shape, dtype)


def local(fields, region_ids, bias_index, earth_bias, w_qkv, w_proj, w_fc1, w_fc2):
    fields = fields.reshape(36, 24, C)
    region = region_ids.transpose(1, 0, 2)
    tables = earth_bias.transpose(0, 2, 1)
    nq, comb, pay, own = call(
        prep_body,
        (sds((6, 160, C), BF16), sds((8, 512), F32), sds((544, C), BF16), sds((CHUNKS, 16, 256), F32)),
        [pltpu.VMEM((6, 160, C), F32), pltpu.VMEM((36, 24), F32), pltpu.VMEM((36, 24, C), BF16),
         pltpu.VMEM((18, 2, 24), jnp.int32), pltpu.VMEM((HEADS, POSITIONS), BF16), pltpu.SemaphoreType.DMA((3,))],
        tuple(hold(x) for x in (fields, region, tables)),
        in_specs=[pl.BlockSpec(memory_space=pltpu.HBM)] * 3,
    )
    lat = shift(pay, "lat", 1)

    kinds = (BF16, BF16, BF16, F32, BF16)
    consts = tuple(jnp.asarray(c, k) for c, k in zip(index_constants(), kinds))
    *found, inner = call(
        index_body,
        (sds((144, 128), F32), sds((144, 128), F32), sds((32, 256), F32), sds((32, 256), F32),
         sds((CHUNKS, 24, 256), F32)),
        [pltpu.VMEM((144, 144), jnp.int32), pltpu.VMEM((2, HEADS, POSITIONS), BF16)] +
        [pltpu.VMEM(c.shape, c.dtype) for c in consts] + [pltpu.SemaphoreType.DMA((7,))],
        tuple(hold(x) for x in (bias_index, tables) + consts),
        in_specs=[pl.BlockSpec(memory_space=pltpu.HBM)] * 7,
        cost_estimate=pl.CostEstimate(flops=10 ** 9, transcendentals=0, bytes_accessed=10 ** 6),
    )

    def bias(late, extra):
        return call(
            lambda *refs: bias_body(late, *refs),
            (sds((ROWS * SPAN, 128), F32),) * 4,
            [pltpu.VMEM((CHUNKS * ROWS, 256), F32)],
            tuple(found) + (own, inner, lat) + extra,
            cost_estimate=pl.CostEstimate(flops=10 ** 10, transcendentals=0,
                                          bytes_accessed=8 * 10 ** 6),
            input_output_aliases={7 + n: n for n in range(4)} if late else {},
        )

    pay_r = call(right_body, sds((336, C), BF16), [pltpu.VMEM((320, C), F32)], (nq, lat, comb))
    left = shift(pay_r, "lon", 1)
    some = bias(False, ())
    pay_l = call(
        left_body,
        sds((320, C), BF16),
        [pltpu.VMEM((320, C), F32)],
        (nq, lat, some[0]),
        in_specs=[pl.BlockSpec(memory_space=pltpu.VMEM)] * 2 + [pl.BlockSpec(memory_space=pl.ANY)],
    )
    right = shift(pay_l, "lon", -1)
    bm0, br0, bm1, br1 = bias(True, tuple(some))
    vm = pltpu.VMEM
    work = [vm((8, 256), F32), vm((KEYS, 128), F32), vm((KEYS, 128), F32)]
    qq, mid = call(
        inner_body,
        (sds((6, 160, C), F32), sds((6, SPAN, C), F32)),
        [vm((640, C), F32), vm((640, C), BF16), vm((640, C), BF16)] + work +
        [vm((2, 960, KEYS), F32), vm((2, 960, 128), F32)],
        (nq, lat, comb, bm1, br1, bm0, br0, w_qkv),
        cost_estimate=pl.CostEstimate(flops=5 * 10 ** 9, transcendentals=0, bytes_accessed=8 * 10 ** 6),
    )
    result = call(
        outer_body,
        sds((36, 24, C), BF16),
        [vm((1280, C), F32), vm((1280, C), BF16), vm((1280, C), BF16), vm((6, 160, C), F32), vm((6, 160, C), F32),
         work[0], vm((36, 24, C), F32)] + work[1:] + [vm((2, 960, KEYS), F32), vm((2, 960, 128), F32)],
        (fields, nq, lat, left, right, comb, qq, mid, bm1, br1, bm0, br0, w_qkv, w_proj, w_fc1, w_fc2),
    )
    return result.reshape(2, 18, 24, C)


def solution(mesh):
    return jax.shard_map(
        local,
        mesh=mesh,
        in_specs=(
            P("ens", "lat", "lon", None),
            P(None, "lat", "lon"),
            P(),
            P("lat", None, None),
            P(),
            P(),
            P(),
            P(),
        ),
        out_specs=P("ens", "lat", "lon", None),
        check_vma=False,
    )
```

```python
import numpy as np
import jax
import jax.numpy as jnp
from jax import lax
from jax.experimental import pallas as pl
from jax.experimental.pallas import tpu as pltpu
from jax.sharding import PartitionSpec as P

F32 = jnp.float32
BF16 = jnp.bfloat16
EPS = 1e-05
LOG2E = 1.4426950408889634
C = 384
HEADS = 12
KEYS = 144
POSITIONS = 3312
CHUNKS = 13
ROWS = 40
SPAN = 80


def floor_div(x, d):
    return jnp.floor((x + 0.5) * (1.0 / d))


def region_constants():
    lane = lax.broadcasted_iota(jnp.int32, (1, 512), 1).astype(F32)
    w = floor_div(lane, 256)
    p = lane - 256 * w
    r2 = floor_div(p, 72)
    c2 = floor_div(p - 72 * r2, 36)
    kk = p - 72 * r2 - 36 * c2
    valid = p < 144
    level = floor_div(kk, 18)
    r3 = floor_div(kk - 18 * level, 6)
    src = jnp.where(valid, 12 * w + 6 * c2 + kk - 18 * level - 6 * r3, -1.0)
    lane_row = jnp.where(valid, level * 6 + r2 * 3 + r3, -1.0)
    cols = jnp.where(lax.broadcasted_iota(jnp.int32, (24, 512), 0).astype(F32) == src, 1.0, 0.0)
    row = lax.broadcasted_iota(jnp.int32, (36, 1), 0).astype(F32)
    r = floor_div(row, 2)
    row_id = (row - 2 * r) * 6 + r - 6 * floor_div(r, 6)
    keep = jnp.where(row_id == lane_row, 1.0, 0.0)
    at = floor_div(lax.broadcasted_iota(jnp.int32, (1, 36), 1).astype(F32), 12)
    group = jnp.where(lax.broadcasted_iota(jnp.int32, (8, 36), 0).astype(F32) == at, 1.0, 0.0)
    return cols.astype(BF16), keep, group.astype(BF16), jnp.where(valid, 0.0, -1.0)


def spread_table(eb, c):
    n = min(256, POSITIONS - 256 * c)
    got = eb[:, 256 * c:256 * c + n].astype(F32)
    if n < 256:
        got = jnp.concatenate([got, jnp.zeros((HEADS, 256 - n), F32)], axis=1)
    return got


def window_order():
    spots = []
    for r2 in range(2):
        for c2 in range(2):
            for level in range(2):
                for r3 in range(3):
                    for c6 in range(6):
                        spots.append(level * 72 + (r2 * 3 + r3) * 12 + c2 * 6 + c6)
    return np.array(spots)


def index_constants():
    pick = (window_order()[:, None] == np.arange(144)[None]).astype(np.float32)
    tile = (np.arange(16)[:, None] == (np.arange(256) % 16)[None]).astype(np.float32)
    row = np.arange(144)
    keep = ((row % 72 % 16)[:, None] == (np.arange(256) // 16)[None]).astype(np.float32)
    gather = ((8 * (row // 72) + row % 72 // 16)[None] == np.arange(16)[:, None]).astype(np.float32)
    return pick, pick.T, tile, keep, gather


def dot(a, b):
    return jnp.dot(a, b, preferred_element_type=F32)


def normalise(x):
    mean = jnp.mean(x, axis=-1, keepdims=True)
    centred = x - mean
    var = jnp.mean(centred * centred, axis=-1, keepdims=True)
    return (centred * lax.rsqrt(var + EPS)).astype(BF16)


def fetch_all(pairs, sems):
    copies = [pltpu.make_async_copy(a, b, sems.at[n]) for n, (a, b) in enumerate(pairs)]
    for copy in copies:
        copy.start()
    return copies


def prep_body(fields_hbm, region_hbm, eb_hbm, nq, comb, pay, own, xq, reg, fields, region, eb, sems):
    copies = fetch_all(((fields_hbm, fields), (region_hbm, region), (eb_hbm.at[2], eb)), sems)
    for cs in range(4):
        for rt in range(6):
            xq[rt, 40 * cs + 32:40 * cs + 40, :] = jnp.zeros((8, C), F32)

    copies[0].wait()

    def triple(rt, carry):
        for level in range(2):
            for r3 in range(3):
                x = fields[level * 18 + 3 * rt + r3].astype(F32)
                n = normalise(x).astype(F32)
                base = 6 * ((1 - level) * 3 + r3)
                for cs in range(4):
                    xq[rt, 40 * cs + base:40 * cs + base + 6, :] = n[6 * cs:6 * cs + 6, :]
        return carry

    lax.fori_loop(0, 6, triple, 0, unroll=3)
    copies[1].wait()
    for r in range(18):
        reg[2 * r:2 * r + 2, :] = region[r].astype(F32)
    cols, keep, group, fill = region_constants()
    spread = dot(reg[...].astype(BF16), cols) * keep
    rows = dot(group, spread.astype(BF16)) + fill
    comb[...] = rows
    nq[...] = xq[...].astype(BF16)
    pay[0:160, :] = xq[0].astype(BF16)
    pay[160:320, :] = xq[5].astype(BF16)
    last = jnp.concatenate([rows[2:3, 0:256], rows[2:3, 256:512], jnp.zeros((14, 256), F32)], axis=0)
    pay[320:336, 0:256] = last.astype(BF16)
    copies[2].wait()
    for c in range(CHUNKS):
        own[c] = jnp.concatenate([spread_table(eb, c), jnp.zeros((4, 256), F32)], axis=0)
        pay[336 + 16 * c:352 + 16 * c, 0:256] = own[c].astype(BF16)


def column(nq, lat, scr, cs):
    sl = slice(40 * cs, 40 * cs + 40)
    scr[0:40, :] = lat[160:320, :].astype(F32)[sl, :]
    scr[280:320, :] = lat[0:160, :].astype(F32)[sl, :]
    for rt in range(6):
        scr[40 * rt + 40:40 * rt + 80, :] = nq[rt].astype(F32)[sl, :]
    return scr[...].astype(BF16)


def right_body(nq, lat, comb, pay, scr):
    pay[0:320, :] = column(nq, lat, scr, 3)
    top = lat[320:336, 0:256].astype(F32)
    rows = jnp.concatenate([top[1:2, :], comb[0:3, 256:512], jnp.zeros((12, 256), F32)], axis=0)
    pay[320:336, 0:256] = rows.astype(BF16)


def left_body(nq, lat, after, pay, scr):
    pay[...] = column(nq, lat, scr, 0)


def index_body(index_hbm, eb_hbm, *refs):
    consts, (lo_m, hi_m, lo_r, hi_r, inner, index, eb), bufs, sems = refs[:5], refs[5:12], refs[12:17], refs[17]
    copies = fetch_all(((index_hbm, index),) + tuple(zip(consts, bufs)) + ((eb_hbm.at[0:2], eb),), sems)
    for copy in copies[:6]:
        copy.wait()
    pick, place, tile, keep, gather = bufs
    idx = index[...]
    for part, m_ref, r_ref in ((idx & 255, lo_m, lo_r), (idx >> 8, hi_m, hi_r)):
        picked = dot(pick[...], part.astype(F32).astype(BF16)).astype(BF16)
        full = dot(picked, place[...])
        m_ref[...] = full[:, 0:128]
        wide = dot(full[:, 128:144].astype(BF16), tile[...]) * keep[...]
        r_ref[...] = dot(gather[...], wide.astype(BF16))
    copies[6].wait()
    for c in range(CHUNKS):
        inner[c, 0:12, :] = spread_table(eb.at[0], c)
        inner[c, 12:24, :] = spread_table(eb.at[1], c)


def early_blocks():
    lon = lax.axis_index("lon")
    late = (lon == 0) & (lax.axis_index("ens") == 0)
    return jnp.where(late, 2, jnp.maximum(7 - lon % 32, 0))


def bias_body(late, lo_m, hi_m, lo_r, hi_r, own, inner, swap, *refs):
    main0, rem0, main1, rem1, tabs = refs[4:] if late else refs
    low = lax.broadcasted_iota(jnp.int32, (256, 256), 0).astype(F32)
    early = early_blocks()

    def look(table, lo, hi):
        hot = jnp.where(low == lo, 1.0, 0.0).astype(BF16)
        got = dot(table, hot)
        out = got[0:ROWS]
        for c in range(1, CHUNKS):
            out = jnp.where(hi == float(c), got[ROWS * c:ROWS * c + ROWS], out)
        return out * LOG2E

    for c in range(CHUNKS):
        tabs[ROWS * c + 16:ROWS * c + ROWS, :] = inner[c]

    for half, main, rem in ((0, main0, rem0), (1, main1, rem1)):
        for c in range(CHUNKS):
            tabs[ROWS * c:ROWS * c + 16, :] = \
                swap[336 + 16 * c:352 + 16 * c, 0:256].astype(F32) if half else own[c]
        table = tabs[...].astype(BF16)
        done = jnp.clip(early - 4 * half, 0, 4)

        def pairs(block, carry):
            first = 24 * block
            for step in range(12):
                at = 72 * half + first + 2 * step
                lo = jnp.concatenate([lo_m[pl.ds(at, 1), :], lo_m[pl.ds(at + 1, 1), :]], axis=1)
                hi = jnp.concatenate([hi_m[pl.ds(at, 1), :], hi_m[pl.ds(at + 1, 1), :]], axis=1)
                out = look(table, lo, hi)
                spot = first + 2 * step
                spot = spot + jnp.where(spot >= 36, 4, 0)
                main[pl.ds(spot, ROWS, stride=SPAN), :] = out[:, 0:128]
                main[pl.ds(spot + 1, ROWS, stride=SPAN), :] = out[:, 128:256]
            return carry

        if late:
            lax.fori_loop(jnp.minimum(done, 3), 3, pairs, 0)
        else:
            lax.fori_loop(0, jnp.minimum(done, 3), pairs, 0)

        @pl.when(done < 4 if late else done >= 4)
        def _():
            for g in range(5):
                out = look(table, lo_r[8 * half + g:8 * half + g + 1, :], hi_r[8 * half + g:8 * half + g + 1, :])
                for q in range(min(16, 72 - 16 * g)):
                    i = 16 * g + q
                    spot = i + 4 * (i // 36)
                    piece = out[:, 128 * (q // 8):128 * (q // 8) + 128]
                    if q % 8:
                        piece = pltpu.roll(piece, 128 - 16 * (q % 8), axis=1)
                    rem[pl.ds(spot, ROWS, stride=SPAN), :] = piece


SPANS = ((40, 40, 0), (0, 80, 40), (0, 40, 120))
SCALE = 32 ** -0.5 * LOG2E


def head_lanes():
    lane = lax.broadcasted_iota(jnp.int32, (1, 128), 1)
    return lane, [(lane // 32 == h) for h in range(4)]


def put(xs, group, rt, second, block):
    at = 576 * group + 72 * rt + 36 * second
    xs[at:at + 36, :] = block[0:36, :]


def key_values(xs, kk, vv, w_qkv, count):
    def project(step, carry):
        at = pl.multiple_of(step * 288, 288)
        y = dot(xs[pl.ds(at, 288), :].astype(BF16), w_qkv[:, C:3 * C])
        kk[pl.ds(at, 288), :] = y[:, 0:C].astype(BF16)
        vv[pl.ds(at, 288), :] = y[:, C:2 * C].astype(BF16)
        return carry

    lax.fori_loop(0, count, project, 0, unroll=count)


def region_features(rows, qf, kf):
    sub = lax.broadcasted_iota(jnp.int32, (8, KEYS), 0).astype(F32)
    hot = jnp.concatenate([jnp.where(sub == rows[n:n + 1, 0:KEYS], 1.0, 0.0) for n in range(8)], axis=0)
    eye = lax.broadcasted_iota(jnp.int32, (64, 128), 0) == lax.broadcasted_iota(jnp.int32, (64, 128), 1)
    seen = lax.dot_general(
        jnp.concatenate([hot, jnp.zeros((64, KEYS), F32)], axis=0).astype(BF16),
        jnp.concatenate([jnp.where(eye, 1.0, 0.0), jnp.zeros((64, 128), F32)], axis=0).astype(BF16),
        (((0,), (0,)), ((), ())), preferred_element_type=F32)
    qf[...] = jnp.zeros((160, 128), F32)
    for n in range(4):
        qf[40 * n:40 * n + 36, :] = seen[36 * n:36 * n + 36, :]
    kf[...] = (seen - 1.0) * 1e30


def attention(windows, tables, qq, kk, vv, qf, kf, sc, mx, store):
    lane, heads = head_lanes()
    ones = jnp.ones((KEYS, 128), BF16)

    def places(r2, step):
        return (step, 2 * step + 1) if r2 else (step + 1, 2 * step + 2)

    def score(r2, step):
        t, rt = places(r2, step)
        if r2:
            th0 = jnp.where(step == 0, 0, 4 + 12 * step)
        else:
            th0 = jnp.where(step == 2, 0, 16 + 12 * step)
        bm, br = tables[r2]
        top = 0
        for n, w in enumerate(windows):
            c0, nrow, q0 = SPANS[w]
            far = jnp.where(lane // 8 == 4 * n + t, kf[...], 0.0).astype(BF16)
            near = qf[80 * r2 + c0:80 * r2 + c0 + nrow, :]
            for g in range(3):
                sl = slice(128 * g, 128 * g + 128)
                k = jnp.concatenate([kk[pl.ds(pl.multiple_of(576 * n + 144 * t, 144), KEYS), sl], far], axis=1)
                q = qq[rt - 1, q0:q0 + nrow, sl]
                qs = jnp.concatenate([jnp.concatenate([jnp.where(m, q, 0.0), near], axis=1) for m in heads],
                                     axis=0).astype(BF16)
                s = lax.dot_general(qs, k, (((1,), (1,)), ((), ())), preferred_element_type=F32)
                for h in range(4):
                    th = pl.multiple_of((th0 + 4 * g + h) * SPAN, SPAN) + c0
                    b = jnp.concatenate([bm[pl.ds(th, nrow), :], br[pl.ds(th, nrow), :][:, 0:16]], axis=1)
                    x = s[h * nrow:(h + 1) * nrow, :] * SCALE + b
                    sc[r2, top:top + nrow, :] = x
                    mx[r2, top:top + nrow, :] = jnp.broadcast_to(jnp.max(x, axis=1, keepdims=True), (nrow, 128))
                    top += nrow

    def attend(r2, step):
        t, rt = places(r2, step)
        top = 0
        for n, w in enumerate(windows):
            _, nrow, _ = SPANS[w]
            for g in range(3):
                sl = slice(128 * g, 128 * g + 128)
                parts = []
                for _ in range(4):
                    m = mx[r2, top:top + nrow, :]
                    x = sc[r2, top:top + nrow, :] - jnp.concatenate([m, m[:, 0:16]], axis=1)
                    parts.append(jnp.exp2(x).astype(BF16))
                    top += nrow
                v = vv[pl.ds(pl.multiple_of(576 * n + 144 * t, 144), KEYS), sl]
                o = dot(jnp.concatenate(parts, axis=0), jnp.concatenate([v, ones], axis=1))
                os = [o[h * nrow:(h + 1) * nrow, :] for h in range(4)]
                num, den = os[3][:, 0:128], os[3][:, 128:256]
                for h in range(3):
                    num = jnp.where(heads[h], os[h][:, 0:128], num)
                    den = jnp.where(heads[h], os[h][:, 128:256], den)
                store(rt - 1, w, sl, num / den)

    score(0, 0)

    def steps(step, carry):
        score(1, step)
        attend(0, step)
        score(0, jnp.minimum(step + 1, 2))
        attend(1, step)
        return carry

    lax.fori_loop(0, 3, steps, 0)


def inner_body(nq, lat, comb, bm1, br1, bm0, br0, w_qkv, qq, ctx, xs, kk, vv, rows, qf, kf, sc, mx):
    for rt in range(8):
        block = lat[160:320, :] if rt == 0 else lat[0:160, :] if rt == 7 else nq[rt - 1]
        block = block.astype(F32)
        put(xs, 0, rt, 0, block[40:80, :])
        put(xs, 0, rt, 1, block[80:120, :])
    key_values(xs, kk, vv, w_qkv, 2)
    for rt in range(6):
        qq[rt] = dot(nq[rt], w_qkv[:, 0:C]).astype(BF16).astype(F32)
    rows[...] = jnp.full((8, 256), -1.0, F32)
    rows[0:1, :] = lat[320:336, 0:256].astype(F32)[0:1, :]
    rows[1:4, :] = comb[0:3, 0:256]
    region_features(rows, qf, kf)

    def store(rt, w, sl, value):
        ctx[rt, :, sl] = value

    attention((1,), ((bm0, br0), (bm1, br1)), qq, kk, vv, qf, kf, sc, mx, store)


def outer_body(fields, nq, lat, left, right, comb, qq, mid, bm1, br1, bm0, br0, w_qkv, w_proj, w_fc1, w_fc2, out,
               xs, kk, vv, ctx, att, rows, res, qf, kf, sc, mx):
    below = lat[0:160, :].astype(F32)
    above = lat[160:320, :].astype(F32)
    put(xs, 0, 0, 1, above[0:40, :])
    put(xs, 1, 0, 0, above[120:160, :])
    put(xs, 0, 7, 1, below[0:40, :])
    put(xs, 1, 7, 0, below[120:160, :])
    lhalo = left[0:320, :].astype(F32)
    rhalo = right[...].astype(F32)
    for rt in range(8):
        put(xs, 0, rt, 0, lhalo[40 * rt:40 * rt + 40, :])
        put(xs, 1, rt, 1, rhalo[40 * rt:40 * rt + 40, :])
    for rt in range(6):
        own = nq[rt].astype(F32)
        put(xs, 0, rt + 1, 1, own[0:40, :])
        put(xs, 1, rt + 1, 0, own[120:160, :])
        ctx[rt, 40:120, :] = mid[rt]
    key_values(xs, kk, vv, w_qkv, 4)
    rows[0:4, :] = left[320:336, 0:256].astype(F32)[0:4, :]
    rows[4:5, :] = lat[320:336, 0:256].astype(F32)[1:2, :]
    rows[5:8, :] = comb[0:3, 256:512]
    region_features(rows, qf, kf)

    def store(rt, w, sl, value):
        ctx[rt, SPANS[w][2]:SPANS[w][2] + 40, sl] = value

    attention((0, 2), ((bm0, br0), (bm1, br1)), qq, kk, vv, qf, kf, sc, mx, store)

    def back(rt, carry):
        att[rt] = dot(ctx[rt].astype(BF16), w_proj[...]).astype(BF16).astype(F32)
        for level in range(2):
            for r3 in range(3):
                base = 6 * ((1 - level) * 3 + r3)
                for cs in range(4):
                    res[level * 18 + 3 * rt + r3, 6 * cs:6 * cs + 6, :] = \
                        att[rt, 40 * cs + base:40 * cs + base + 6, :]
        return carry

    lax.fori_loop(0, 6, back, 0, unroll=6)

    def feed(step, carry):
        x = fields[pl.ds(9 * step, 9)].astype(F32) + res[pl.ds(9 * step, 9)]
        x = x.reshape(216, C).astype(BF16).astype(F32)
        y = dot(normalise(x), w_fc1[...])
        hidden = (0.5 * y * (1.0 + lax.erf(y * (0.5 ** 0.5)))).astype(BF16)
        z = x + dot(hidden, w_fc2[...])
        out[pl.ds(9 * step, 9)] = z.reshape(9, 24, C).astype(BF16)
        return carry

    lax.fori_loop(0, 4, feed, 0, unroll=4)


def call(body, outs, scratch, args, limit=28, **kw):
    return pl.pallas_call(
        body,
        out_shape=outs,
        scratch_shapes=scratch,
        compiler_params=pltpu.CompilerParams(vmem_limit_bytes=limit << 20),
        **kw,
    )(*args)


def hold(x):
    return pltpu.with_memory_space_constraint(x, pltpu.HBM)


def shift(value, axis, steps):
    count = lax.axis_size(axis)
    return lax.ppermute(value, axis, [(s, (s + steps) % count) for s in range(count)])


def sds(shape, dtype):
    return jax.ShapeDtypeStruct(shape, dtype)


def local(fields, region_ids, bias_index, earth_bias, w_qkv, w_proj, w_fc1, w_fc2):
    fields = fields.reshape(36, 24, C)
    region = region_ids.transpose(1, 0, 2)
    tables = earth_bias.transpose(0, 2, 1)
    nq, comb, pay, own = call(
        prep_body,
        (sds((6, 160, C), BF16), sds((8, 512), F32), sds((544, C), BF16), sds((CHUNKS, 16, 256), F32)),
        [pltpu.VMEM((6, 160, C), F32), pltpu.VMEM((36, 24), F32), pltpu.VMEM((36, 24, C), BF16),
         pltpu.VMEM((18, 2, 24), jnp.int32), pltpu.VMEM((HEADS, POSITIONS), BF16), pltpu.SemaphoreType.DMA((3,))],
        tuple(hold(x) for x in (fields, region, tables)),
        in_specs=[pl.BlockSpec(memory_space=pltpu.HBM)] * 3,
    )
    lat = shift(pay, "lat", 1)

    kinds = (BF16, BF16, BF16, F32, BF16)
    consts = tuple(jnp.asarray(c, k) for c, k in zip(index_constants(), kinds))
    *found, inner = call(
        index_body,
        (sds((144, 128), F32), sds((144, 128), F32), sds((16, 256), F32), sds((16, 256), F32),
         sds((CHUNKS, 24, 256), F32)),
        [pltpu.VMEM((144, 144), jnp.int32), pltpu.VMEM((2, HEADS, POSITIONS), BF16)] +
        [pltpu.VMEM(c.shape, c.dtype) for c in consts] + [pltpu.SemaphoreType.DMA((7,))],
        tuple(hold(x) for x in (bias_index, tables) + consts),
        in_specs=[pl.BlockSpec(memory_space=pltpu.HBM)] * 7,
        cost_estimate=pl.CostEstimate(flops=10 ** 9, transcendentals=0, bytes_accessed=10 ** 6),
    )

    def bias(late, extra):
        return call(
            lambda *refs: bias_body(late, *refs),
            (sds((ROWS * SPAN, 128), F32),) * 4,
            [pltpu.VMEM((CHUNKS * ROWS, 256), F32)],
            tuple(found) + (own, inner, lat) + extra,
            cost_estimate=pl.CostEstimate(flops=10 ** 10, transcendentals=0,
                                          bytes_accessed=8 * 10 ** 6),
            input_output_aliases={7 + n: n for n in range(4)} if late else {},
        )

    pay_r = call(right_body, sds((336, C), BF16), [pltpu.VMEM((320, C), F32)], (nq, lat, comb))
    left = shift(pay_r, "lon", 1)
    some = bias(False, ())
    pay_l = call(
        left_body,
        sds((320, C), BF16),
        [pltpu.VMEM((320, C), F32)],
        (nq, lat, some[0]),
        in_specs=[pl.BlockSpec(memory_space=pltpu.VMEM)] * 2 + [pl.BlockSpec(memory_space=pl.ANY)],
    )
    right = shift(pay_l, "lon", -1)
    bm0, br0, bm1, br1 = bias(True, tuple(some))
    vm = pltpu.VMEM
    work = [vm((8, 256), F32), vm((160, 128), F32), vm((KEYS, 128), F32)]
    qq, mid = call(
        inner_body,
        (sds((6, 160, C), F32), sds((6, SPAN, C), F32)),
        [vm((576, C), F32), vm((576, C), BF16), vm((576, C), BF16)] + work +
        [vm((2, 960, KEYS), F32), vm((2, 960, 128), F32)],
        (nq, lat, comb, bm1, br1, bm0, br0, w_qkv),
        cost_estimate=pl.CostEstimate(flops=5 * 10 ** 9, transcendentals=0, bytes_accessed=8 * 10 ** 6),
    )
    result = call(
        outer_body,
        sds((36, 24, C), BF16),
        [vm((1152, C), F32), vm((1152, C), BF16), vm((1152, C), BF16), vm((6, 160, C), F32), vm((6, 160, C), F32),
         work[0], vm((36, 24, C), F32)] + work[1:] + [vm((2, 960, KEYS), F32), vm((2, 960, 128), F32)],
        (fields, nq, lat, left, right, comb, qq, mid, bm1, br1, bm0, br0, w_qkv, w_proj, w_fc1, w_fc2),
    )
    return result.reshape(2, 18, 24, C)


def solution(mesh):
    return jax.shard_map(
        local,
        mesh=mesh,
        in_specs=(
            P("ens", "lat", "lon", None),
            P(None, "lat", "lon"),
            P(),
            P("lat", None, None),
            P(),
            P(),
            P(),
            P(),
        ),
        out_specs=P("ens", "lat", "lon", None),
        check_vma=False,
    )
```

```python
import numpy as np
import jax
import jax.numpy as jnp
from jax import lax
from jax.experimental import pallas as pl
from jax.experimental.pallas import tpu as pltpu
from jax.sharding import PartitionSpec as P

F32 = jnp.float32
BF16 = jnp.bfloat16
EPS = 1e-05
LOG2E = 1.4426950408889634
C = 384
HEADS = 12
KEYS = 144
POSITIONS = 3312
CHUNKS = 13
ROWS = 40
SPAN = 80


def floor_div(x, d):
    return jnp.floor((x + 0.5) * (1.0 / d))


def region_constants():
    lane = lax.broadcasted_iota(jnp.int32, (1, 512), 1).astype(F32)
    w = floor_div(lane, 256)
    p = lane - 256 * w
    r2 = floor_div(p, 72)
    c2 = floor_div(p - 72 * r2, 36)
    kk = p - 72 * r2 - 36 * c2
    valid = p < 144
    level = floor_div(kk, 18)
    r3 = floor_div(kk - 18 * level, 6)
    src = jnp.where(valid, 12 * w + 6 * c2 + kk - 18 * level - 6 * r3, -1.0)
    lane_row = jnp.where(valid, level * 6 + r2 * 3 + r3, -1.0)
    cols = jnp.where(lax.broadcasted_iota(jnp.int32, (24, 512), 0).astype(F32) == src, 1.0, 0.0)
    row = lax.broadcasted_iota(jnp.int32, (36, 1), 0).astype(F32)
    r = floor_div(row, 2)
    row_id = (row - 2 * r) * 6 + r - 6 * floor_div(r, 6)
    keep = jnp.where(row_id == lane_row, 1.0, 0.0)
    at = floor_div(lax.broadcasted_iota(jnp.int32, (1, 36), 1).astype(F32), 12)
    group = jnp.where(lax.broadcasted_iota(jnp.int32, (8, 36), 0).astype(F32) == at, 1.0, 0.0)
    return cols.astype(BF16), keep, group.astype(BF16), jnp.where(valid, 0.0, -1.0)


def spread_table(eb, c):
    n = min(256, POSITIONS - 256 * c)
    got = eb[:, 256 * c:256 * c + n].astype(F32)
    if n < 256:
        got = jnp.concatenate([got, jnp.zeros((HEADS, 256 - n), F32)], axis=1)
    return got


def window_order():
    spots = []
    for r2 in range(2):
        for c2 in range(2):
            for level in range(2):
                for r3 in range(3):
                    for c6 in range(6):
                        spots.append(level * 72 + (r2 * 3 + r3) * 12 + c2 * 6 + c6)
    return np.array(spots)


def index_constants():
    pick = (window_order()[:, None] == np.arange(144)[None]).astype(np.float32)
    tile = (np.arange(16)[:, None] == (np.arange(256) % 16)[None]).astype(np.float32)
    row = np.arange(144)
    keep = ((row % 72 % 16)[:, None] == (np.arange(256) // 16)[None]).astype(np.float32)
    gather = ((8 * (row // 72) + row % 72 // 16)[None] == np.arange(16)[:, None]).astype(np.float32)
    return pick, pick.T, tile, keep, gather


def dot(a, b):
    return jnp.dot(a, b, preferred_element_type=F32)


def normalise(x):
    mean = jnp.mean(x, axis=-1, keepdims=True)
    centred = x - mean
    var = jnp.mean(centred * centred, axis=-1, keepdims=True)
    return (centred * lax.rsqrt(var + EPS)).astype(BF16)


def fetch_all(pairs, sems):
    copies = [pltpu.make_async_copy(a, b, sems.at[n]) for n, (a, b) in enumerate(pairs)]
    for copy in copies:
        copy.start()
    return copies


def prep_body(fields_hbm, region_hbm, eb_hbm, index_hbm, *refs):
    consts, (nq, comb, pay, own, lo_m, hi_m, lo_r, hi_r, inner) = refs[:5], refs[5:14]
    (xq, reg, fields, region, eb, index), bufs, sems = refs[14:20], refs[20:25], refs[25]
    copies = fetch_all(((fields_hbm, fields), (region_hbm, region), (eb_hbm, eb), (index_hbm, index)) +
                       tuple(zip(consts, bufs)), sems)
    for cs in range(4):
        for rt in range(6):
            xq[rt, 40 * cs + 32:40 * cs + 40, :] = jnp.zeros((8, C), F32)

    copies[0].wait()

    def triple(rt, carry):
        for level in range(2):
            for r3 in range(3):
                x = fields[level * 18 + 3 * rt + r3].astype(F32)
                n = normalise(x).astype(F32)
                base = 6 * ((1 - level) * 3 + r3)
                for cs in range(4):
                    xq[rt, 40 * cs + base:40 * cs + base + 6, :] = n[6 * cs:6 * cs + 6, :]
        return carry

    lax.fori_loop(0, 6, triple, 0, unroll=3)
    copies[1].wait()
    for r in range(18):
        reg[2 * r:2 * r + 2, :] = region[r].astype(F32)
    cols, keep, group, fill = region_constants()
    spread = dot(reg[...].astype(BF16), cols) * keep
    rows = dot(group, spread.astype(BF16)) + fill
    comb[...] = rows
    nq[...] = xq[...].astype(BF16)
    pay[0:160, :] = xq[0].astype(BF16)
    pay[160:320, :] = xq[5].astype(BF16)
    last = jnp.concatenate([rows[2:3, 0:256], rows[2:3, 256:512], jnp.zeros((14, 256), F32)], axis=0)
    pay[320:336, 0:256] = last.astype(BF16)
    copies[2].wait()
    for c in range(CHUNKS):
        own[c] = jnp.concatenate([spread_table(eb.at[2], c), jnp.zeros((4, 256), F32)], axis=0)
        pay[336 + 16 * c:352 + 16 * c, 0:256] = own[c].astype(BF16)
        inner[c, 0:12, :] = spread_table(eb.at[0], c)
        inner[c, 12:24, :] = spread_table(eb.at[1], c)
    for copy in copies[3:]:
        copy.wait()
    pick, place, tile, keep, gather = bufs
    idx = index[...]
    for part, m_ref, r_ref in ((idx & 255, lo_m, lo_r), (idx >> 8, hi_m, hi_r)):
        picked = dot(pick[...], part.astype(F32).astype(BF16)).astype(BF16)
        full = dot(picked, place[...])
        m_ref[...] = full[:, 0:128]
        wide = dot(full[:, 128:144].astype(BF16), tile[...]) * keep[...]
        r_ref[...] = dot(gather[...], wide.astype(BF16))


def column(nq, lat, scr, cs):
    sl = slice(40 * cs, 40 * cs + 40)
    scr[0:40, :] = lat[160:320, :].astype(F32)[sl, :]
    scr[280:320, :] = lat[0:160, :].astype(F32)[sl, :]
    for rt in range(6):
        scr[40 * rt + 40:40 * rt + 80, :] = nq[rt].astype(F32)[sl, :]
    return scr[...].astype(BF16)


def right_body(nq, lat, comb, pay, scr):
    pay[0:320, :] = column(nq, lat, scr, 3)
    top = lat[320:336, 0:256].astype(F32)
    rows = jnp.concatenate([top[1:2, :], comb[0:3, 256:512], jnp.zeros((12, 256), F32)], axis=0)
    pay[320:336, 0:256] = rows.astype(BF16)


def left_body(nq, lat, after, pay, scr):
    pay[...] = column(nq, lat, scr, 0)


def block_range(stage):
    lon = lax.axis_index("lon")
    first = jnp.where((lon == 0) & (lax.axis_index("lat") == 1) & (lax.axis_index("ens") == 0), 4, 0)
    second = jnp.maximum(first, 2)
    third = jnp.maximum(second, 8 - lon % 32)
    return ((0, first), (first, second), (second, third), (third, 8))[stage]


def bias_body(stage, lo_m, hi_m, lo_r, hi_r, own, inner, swap, *refs):
    main0, rem0, main1, rem1, tabs = (refs[0:4] + refs[-1:]) if stage == 0 else refs[-5:]
    begin, end = block_range(stage)
    low = lax.broadcasted_iota(jnp.int32, (256, 256), 0).astype(F32)

    def look(table, lo, hi):
        hot = jnp.where(low == lo, 1.0, 0.0).astype(BF16)
        got = dot(table, hot)
        out = got[0:ROWS]
        for c in range(1, CHUNKS):
            out = jnp.where(hi == float(c), got[ROWS * c:ROWS * c + ROWS], out)
        return out * LOG2E

    for c in range(CHUNKS):
        tabs[ROWS * c + 16:ROWS * c + ROWS, :] = inner[c]

    for half, main, rem in ((0, main0, rem0), (1, main1, rem1))[:1 if stage < 2 else 2]:
        for c in range(CHUNKS):
            tabs[ROWS * c:ROWS * c + 16, :] = \
                swap[336 + 16 * c:352 + 16 * c, 0:256].astype(F32) if half else own[c]
        table = tabs[...].astype(BF16)

        def pairs(block, carry):
            first = 24 * block
            for step in range(12):
                at = 72 * half + first + 2 * step
                lo = jnp.concatenate([lo_m[pl.ds(at, 1), :], lo_m[pl.ds(at + 1, 1), :]], axis=1)
                hi = jnp.concatenate([hi_m[pl.ds(at, 1), :], hi_m[pl.ds(at + 1, 1), :]], axis=1)
                out = look(table, lo, hi)
                spot = first + 2 * step
                spot = spot + jnp.where(spot >= 36, 4, 0)
                main[pl.ds(spot, ROWS, stride=SPAN), :] = out[:, 0:128]
                main[pl.ds(spot + 1, ROWS, stride=SPAN), :] = out[:, 128:256]
            return carry

        lax.fori_loop(jnp.clip(begin - 4 * half, 0, 3), jnp.clip(end - 4 * half, 0, 3), pairs, 0)

        @pl.when((begin <= 4 * half + 3) & (end > 4 * half + 3))
        def _():
            for g in range(5):
                out = look(table, lo_r[8 * half + g:8 * half + g + 1, :], hi_r[8 * half + g:8 * half + g + 1, :])
                for q in range(min(16, 72 - 16 * g)):
                    i = 16 * g + q
                    spot = i + 4 * (i // 36)
                    piece = out[:, 128 * (q // 8):128 * (q // 8) + 128]
                    if q % 8:
                        piece = pltpu.roll(piece, 128 - 16 * (q % 8), axis=1)
                    rem[pl.ds(spot, ROWS, stride=SPAN), :] = piece


SPANS = ((40, 40, 0), (0, 80, 40), (0, 40, 120))
SCALE = 32 ** -0.5 * LOG2E


def head_lanes():
    lane = lax.broadcasted_iota(jnp.int32, (1, 128), 1)
    return lane, [(lane // 32 == h) for h in range(4)]


def put(xs, group, rt, second, block):
    at = 576 * group + 72 * rt + 36 * second
    xs[at:at + 36, :] = block[0:36, :]


def key_values(xs, kk, vv, w_qkv, count):
    def project(step, carry):
        at = pl.multiple_of(step * 288, 288)
        y = dot(xs[pl.ds(at, 288), :].astype(BF16), w_qkv[:, C:3 * C])
        kk[pl.ds(at, 288), :] = y[:, 0:C].astype(BF16)
        vv[pl.ds(at, 288), :] = y[:, C:2 * C].astype(BF16)
        return carry

    lax.fori_loop(0, count, project, 0, unroll=count)


def region_features(rows, qf, kf):
    sub = lax.broadcasted_iota(jnp.int32, (8, KEYS), 0).astype(F32)
    hot = jnp.concatenate([jnp.where(sub == rows[n:n + 1, 0:KEYS], 1.0, 0.0) for n in range(8)], axis=0)
    eye = lax.broadcasted_iota(jnp.int32, (64, 128), 0) == lax.broadcasted_iota(jnp.int32, (64, 128), 1)
    seen = lax.dot_general(
        jnp.concatenate([hot, jnp.zeros((64, KEYS), F32)], axis=0).astype(BF16),
        jnp.concatenate([jnp.where(eye, 1.0, 0.0), jnp.zeros((64, 128), F32)], axis=0).astype(BF16),
        (((0,), (0,)), ((), ())), preferred_element_type=F32)
    qf[...] = jnp.zeros((160, 128), F32)
    for n in range(4):
        qf[40 * n:40 * n + 36, :] = seen[36 * n:36 * n + 36, :]
    kf[...] = (seen - 1.0) * 1e30


def attention(windows, tables, qq, kk, vv, qf, kf, sc, mx, store):
    lane, heads = head_lanes()
    ones = jnp.ones((KEYS, 128), BF16)

    def places(r2, step):
        return (step, 2 * step + 1) if r2 else (step + 1, 2 * step + 2)

    def score(r2, step):
        t, rt = places(r2, step)
        if r2:
            th0 = jnp.where(step == 0, 0, 4 + 12 * step)
        else:
            th0 = jnp.where(step == 2, 0, 16 + 12 * step)
        bm, br = tables[r2]
        top = 0
        for n, w in enumerate(windows):
            c0, nrow, q0 = SPANS[w]
            far = jnp.where(lane // 8 == 4 * n + t, kf[...], 0.0).astype(BF16)
            near = qf[80 * r2 + c0:80 * r2 + c0 + nrow, :]
            for g in range(3):
                sl = slice(128 * g, 128 * g + 128)
                k = jnp.concatenate([kk[pl.ds(pl.multiple_of(576 * n + 144 * t, 144), KEYS), sl], far], axis=1)
                q = qq[rt - 1, q0:q0 + nrow, sl]
                qs = jnp.concatenate([jnp.concatenate([jnp.where(m, q, 0.0), near], axis=1) for m in heads],
                                     axis=0).astype(BF16)
                s = lax.dot_general(qs, k, (((1,), (1,)), ((), ())), preferred_element_type=F32)
                for h in range(4):
                    th = pl.multiple_of((th0 + 4 * g + h) * SPAN, SPAN) + c0
                    b = jnp.concatenate([bm[pl.ds(th, nrow), :], br[pl.ds(th, nrow), :][:, 0:16]], axis=1)
                    x = s[h * nrow:(h + 1) * nrow, :] * SCALE + b
                    sc[r2, top:top + nrow, :] = x
                    mx[r2, top:top + nrow, :] = jnp.broadcast_to(jnp.max(x, axis=1, keepdims=True), (nrow, 128))
                    top += nrow

    def attend(r2, step):
        t, rt = places(r2, step)
        top = 0
        for n, w in enumerate(windows):
            _, nrow, _ = SPANS[w]
            for g in range(3):
                sl = slice(128 * g, 128 * g + 128)
                parts = []
                for _ in range(4):
                    m = mx[r2, top:top + nrow, :]
                    x = sc[r2, top:top + nrow, :] - jnp.concatenate([m, m[:, 0:16]], axis=1)
                    parts.append(jnp.exp2(x).astype(BF16))
                    top += nrow
                v = vv[pl.ds(pl.multiple_of(576 * n + 144 * t, 144), KEYS), sl]
                o = dot(jnp.concatenate(parts, axis=0), jnp.concatenate([v, ones], axis=1))
                os = [o[h * nrow:(h + 1) * nrow, :] for h in range(4)]
                num, den = os[3][:, 0:128], os[3][:, 128:256]
                for h in range(3):
                    num = jnp.where(heads[h], os[h][:, 0:128], num)
                    den = jnp.where(heads[h], os[h][:, 128:256], den)
                store(rt - 1, w, sl, num / den)

    score(0, 0)

    def steps(step, carry):
        score(1, step)
        attend(0, step)
        score(0, jnp.minimum(step + 1, 2))
        attend(1, step)
        return carry

    lax.fori_loop(0, 3, steps, 0)


def inner_body(nq, lat, comb, bm1, br1, bm0, br0, w_qkv, qq, ctx, xs, kk, vv, rows, qf, kf, sc, mx):
    for rt in range(8):
        block = lat[160:320, :] if rt == 0 else lat[0:160, :] if rt == 7 else nq[rt - 1]
        block = block.astype(F32)
        put(xs, 0, rt, 0, block[40:80, :])
        put(xs, 0, rt, 1, block[80:120, :])
    key_values(xs, kk, vv, w_qkv, 2)
    for rt in range(6):
        qq[rt] = dot(nq[rt], w_qkv[:, 0:C]).astype(BF16).astype(F32)
    rows[...] = jnp.full((8, 256), -1.0, F32)
    rows[0:1, :] = lat[320:336, 0:256].astype(F32)[0:1, :]
    rows[1:4, :] = comb[0:3, 0:256]
    region_features(rows, qf, kf)

    def store(rt, w, sl, value):
        ctx[rt, :, sl] = value

    attention((1,), ((bm0, br0), (bm1, br1)), qq, kk, vv, qf, kf, sc, mx, store)


def outer_body(fields, nq, lat, left, right, comb, qq, mid, bm1, br1, bm0, br0, w_qkv, w_proj, w_fc1, w_fc2, out,
               xs, kk, vv, ctx, att, rows, res, qf, kf, sc, mx):
    below = lat[0:160, :].astype(F32)
    above = lat[160:320, :].astype(F32)
    put(xs, 0, 0, 1, above[0:40, :])
    put(xs, 1, 0, 0, above[120:160, :])
    put(xs, 0, 7, 1, below[0:40, :])
    put(xs, 1, 7, 0, below[120:160, :])
    lhalo = left[0:320, :].astype(F32)
    rhalo = right[...].astype(F32)
    for rt in range(8):
        put(xs, 0, rt, 0, lhalo[40 * rt:40 * rt + 40, :])
        put(xs, 1, rt, 1, rhalo[40 * rt:40 * rt + 40, :])
    for rt in range(6):
        own = nq[rt].astype(F32)
        put(xs, 0, rt + 1, 1, own[0:40, :])
        put(xs, 1, rt + 1, 0, own[120:160, :])
        ctx[rt, 40:120, :] = mid[rt]
    key_values(xs, kk, vv, w_qkv, 4)
    rows[0:4, :] = left[320:336, 0:256].astype(F32)[0:4, :]
    rows[4:5, :] = lat[320:336, 0:256].astype(F32)[1:2, :]
    rows[5:8, :] = comb[0:3, 256:512]
    region_features(rows, qf, kf)

    def store(rt, w, sl, value):
        ctx[rt, SPANS[w][2]:SPANS[w][2] + 40, sl] = value

    attention((0, 2), ((bm0, br0), (bm1, br1)), qq, kk, vv, qf, kf, sc, mx, store)

    def back(rt, carry):
        att[rt] = dot(ctx[rt].astype(BF16), w_proj[...]).astype(BF16).astype(F32)
        for level in range(2):
            for r3 in range(3):
                base = 6 * ((1 - level) * 3 + r3)
                for cs in range(4):
                    res[level * 18 + 3 * rt + r3, 6 * cs:6 * cs + 6, :] = \
                        att[rt, 40 * cs + base:40 * cs + base + 6, :]
        return carry

    lax.fori_loop(0, 6, back, 0, unroll=6)

    def feed(step, carry):
        x = fields[pl.ds(9 * step, 9)].astype(F32) + res[pl.ds(9 * step, 9)]
        x = x.reshape(216, C).astype(BF16).astype(F32)
        y = dot(normalise(x), w_fc1[...])
        hidden = (0.5 * y * (1.0 + lax.erf(y * (0.5 ** 0.5)))).astype(BF16)
        z = x + dot(hidden, w_fc2[...])
        out[pl.ds(9 * step, 9)] = z.reshape(9, 24, C).astype(BF16)
        return carry

    lax.fori_loop(0, 4, feed, 0, unroll=4)


def call(body, outs, scratch, args, limit=28, **kw):
    return pl.pallas_call(
        body,
        out_shape=outs,
        scratch_shapes=scratch,
        compiler_params=pltpu.CompilerParams(vmem_limit_bytes=limit << 20),
        **kw,
    )(*args)


def hold(x):
    return pltpu.with_memory_space_constraint(x, pltpu.HBM)


def shift(value, axis, steps):
    count = lax.axis_size(axis)
    return lax.ppermute(value, axis, [(s, (s + steps) % count) for s in range(count)])


def sds(shape, dtype):
    return jax.ShapeDtypeStruct(shape, dtype)


def local(fields, region_ids, bias_index, earth_bias, w_qkv, w_proj, w_fc1, w_fc2):
    fields = fields.reshape(36, 24, C)
    region = region_ids.transpose(1, 0, 2)
    tables = earth_bias.transpose(0, 2, 1)
    vm = pltpu.VMEM
    kinds = (BF16, BF16, BF16, F32, BF16)
    consts = tuple(jnp.asarray(c, k) for c, k in zip(index_constants(), kinds))
    nq, comb, pay, own, *found, inner = call(
        prep_body,
        (sds((6, 160, C), BF16), sds((8, 512), F32), sds((544, C), BF16), sds((CHUNKS, 16, 256), F32),
         sds((144, 128), F32), sds((144, 128), F32), sds((16, 256), F32), sds((16, 256), F32),
         sds((CHUNKS, 24, 256), F32)),
        [vm((6, 160, C), F32), vm((36, 24), F32), vm((36, 24, C), BF16), vm((18, 2, 24), jnp.int32),
         vm((3, HEADS, POSITIONS), BF16), vm((144, 144), jnp.int32)] +
        [vm(c.shape, c.dtype) for c in consts] + [pltpu.SemaphoreType.DMA((9,))],
        tuple(hold(x) for x in (fields, region, tables, bias_index) + consts),
        in_specs=[pl.BlockSpec(memory_space=pltpu.HBM)] * 9,
    )

    def bias(stage, extra, kept):
        count = len(kept)
        table = (sds((ROWS * SPAN, 128), F32),) * 4
        alias = {7 + n: n for n in range(4)} if stage else {7: 4}
        return call(
            lambda *refs: bias_body(stage, *refs[:7], *refs[7 + count:]),
            table if stage else table + (sds(pay.shape, pay.dtype),),
            [vm((CHUNKS * ROWS, 256), F32)],
            tuple(found) + (own, inner, extra) + kept,
            in_specs=[pl.BlockSpec(memory_space=vm)] * 7 + [pl.BlockSpec(memory_space=vm if stage else pl.ANY)] * count,
            out_specs=tuple([pl.BlockSpec(memory_space=vm)] * 4 + [pl.BlockSpec(memory_space=pl.ANY)] * (not stage)),
            cost_estimate=pl.CostEstimate(flops=10 ** 10 if stage > 1 else 3 * 10 ** 9, transcendentals=0,
                                          bytes_accessed=8 * 10 ** 6),
            input_output_aliases=alias,
        )

    *some, pay = bias(0, own, (pay,))
    lat = shift(pay, "lat", 1)
    some = bias(1, own, tuple(some))
    pay_r = call(right_body, sds((336, C), BF16), [pltpu.VMEM((320, C), F32)], (nq, lat, comb))
    left = shift(pay_r, "lon", 1)
    some = bias(2, lat, tuple(some))
    pay_l = call(
        left_body,
        sds((320, C), BF16),
        [pltpu.VMEM((320, C), F32)],
        (nq, lat, some[0]),
        in_specs=[pl.BlockSpec(memory_space=pltpu.VMEM)] * 2 + [pl.BlockSpec(memory_space=pl.ANY)],
    )
    right = shift(pay_l, "lon", -1)
    bm0, br0, bm1, br1 = bias(3, lat, tuple(some))
    vm = pltpu.VMEM
    work = [vm((8, 256), F32), vm((160, 128), F32), vm((KEYS, 128), F32)]
    qq, mid = call(
        inner_body,
        (sds((6, 160, C), F32), sds((6, SPAN, C), F32)),
        [vm((576, C), F32), vm((576, C), BF16), vm((576, C), BF16)] + work +
        [vm((2, 960, KEYS), F32), vm((2, 960, 128), F32)],
        (nq, lat, comb, bm1, br1, bm0, br0, w_qkv),
        cost_estimate=pl.CostEstimate(flops=5 * 10 ** 9, transcendentals=0, bytes_accessed=8 * 10 ** 6),
    )
    result = call(
        outer_body,
        sds((36, 24, C), BF16),
        [vm((1152, C), F32), vm((1152, C), BF16), vm((1152, C), BF16), vm((6, 160, C), F32), vm((6, 160, C), F32),
         work[0], vm((36, 24, C), F32)] + work[1:] + [vm((2, 960, KEYS), F32), vm((2, 960, 128), F32)],
        (fields, nq, lat, left, right, comb, qq, mid, bm1, br1, bm0, br0, w_qkv, w_proj, w_fc1, w_fc2),
    )
    return result.reshape(2, 18, 24, C)


def solution(mesh):
    return jax.shard_map(
        local,
        mesh=mesh,
        in_specs=(
            P("ens", "lat", "lon", None),
            P(None, "lat", "lon"),
            P(),
            P("lat", None, None),
            P(),
            P(),
            P(),
            P(),
        ),
        out_specs=P("ens", "lat", "lon", None),
        check_vma=False,
    )
```

```python
import numpy as np
import jax
import jax.numpy as jnp
from jax import lax
from jax.experimental import pallas as pl
from jax.experimental.pallas import tpu as pltpu
from jax.sharding import PartitionSpec as P

F32 = jnp.float32
BF16 = jnp.bfloat16
EPS = 1e-05
LOG2E = 1.4426950408889634
C = 384
HEADS = 12
KEYS = 144
POSITIONS = 3312
CHUNKS = 13
ROWS = 40
SPAN = 80


def floor_div(x, d):
    return jnp.floor((x + 0.5) * (1.0 / d))


def region_constants():
    lane = lax.broadcasted_iota(jnp.int32, (1, 512), 1).astype(F32)
    w = floor_div(lane, 256)
    p = lane - 256 * w
    r2 = floor_div(p, 72)
    c2 = floor_div(p - 72 * r2, 36)
    kk = p - 72 * r2 - 36 * c2
    valid = p < 144
    level = floor_div(kk, 18)
    r3 = floor_div(kk - 18 * level, 6)
    src = jnp.where(valid, 12 * w + 6 * c2 + kk - 18 * level - 6 * r3, -1.0)
    lane_row = jnp.where(valid, level * 6 + r2 * 3 + r3, -1.0)
    cols = jnp.where(lax.broadcasted_iota(jnp.int32, (24, 512), 0).astype(F32) == src, 1.0, 0.0)
    row = lax.broadcasted_iota(jnp.int32, (36, 1), 0).astype(F32)
    r = floor_div(row, 2)
    row_id = (row - 2 * r) * 6 + r - 6 * floor_div(r, 6)
    keep = jnp.where(row_id == lane_row, 1.0, 0.0)
    at = floor_div(lax.broadcasted_iota(jnp.int32, (1, 36), 1).astype(F32), 12)
    group = jnp.where(lax.broadcasted_iota(jnp.int32, (8, 36), 0).astype(F32) == at, 1.0, 0.0)
    return cols.astype(BF16), keep, group.astype(BF16), jnp.where(valid, 0.0, -1.0)


def spread_table(eb, c):
    n = min(256, POSITIONS - 256 * c)
    got = eb[:, 256 * c:256 * c + n].astype(F32)
    if n < 256:
        got = jnp.concatenate([got, jnp.zeros((HEADS, 256 - n), F32)], axis=1)
    return got


def window_order():
    spots = []
    for r2 in range(2):
        for c2 in range(2):
            for level in range(2):
                for r3 in range(3):
                    for c6 in range(6):
                        spots.append(level * 72 + (r2 * 3 + r3) * 12 + c2 * 6 + c6)
    return np.array(spots)


def index_constants():
    pick = (window_order()[:, None] == np.arange(144)[None]).astype(np.float32)
    tile = (np.arange(16)[:, None] == (np.arange(256) % 16)[None]).astype(np.float32)
    row = np.arange(144)
    keep = ((row % 72 % 16)[:, None] == (np.arange(256) // 16)[None]).astype(np.float32)
    gather = ((8 * (row // 72) + row % 72 // 16)[None] == np.arange(16)[:, None]).astype(np.float32)
    return pick, pick.T, tile, keep, gather


def dot(a, b):
    return jnp.dot(a, b, preferred_element_type=F32)


def normalise(x):
    mean = jnp.mean(x, axis=-1, keepdims=True)
    centred = x - mean
    var = jnp.mean(centred * centred, axis=-1, keepdims=True)
    return (centred * lax.rsqrt(var + EPS)).astype(BF16)


def fetch_all(pairs, sems):
    copies = [pltpu.make_async_copy(a, b, sems.at[n]) for n, (a, b) in enumerate(pairs)]
    for copy in copies:
        copy.start()
    return copies


def prep_body(fields_hbm, region_hbm, eb_hbm, index_hbm, *refs):
    consts, (nq, comb, pay, own, lo_m, hi_m, lo_r, hi_r, inner) = refs[:5], refs[5:14]
    (xq, reg, fields, region, eb, index), bufs, sems = refs[14:20], refs[20:25], refs[25]
    copies = fetch_all(((fields_hbm, fields), (region_hbm, region), (eb_hbm, eb), (index_hbm, index)) +
                       tuple(zip(consts, bufs)), sems)
    for cs in range(4):
        for rt in range(6):
            xq[rt, 40 * cs + 32:40 * cs + 40, :] = jnp.zeros((8, C), F32)

    copies[0].wait()

    def triple(rt, carry):
        for level in range(2):
            for r3 in range(3):
                x = fields[level * 18 + 3 * rt + r3].astype(F32)
                n = normalise(x).astype(F32)
                base = 6 * ((1 - level) * 3 + r3)
                for cs in range(4):
                    xq[rt, 40 * cs + base:40 * cs + base + 6, :] = n[6 * cs:6 * cs + 6, :]
        return carry

    lax.fori_loop(0, 6, triple, 0, unroll=3)
    copies[1].wait()
    for r in range(18):
        reg[2 * r:2 * r + 2, :] = region[r].astype(F32)
    cols, keep, group, fill = region_constants()
    spread = dot(reg[...].astype(BF16), cols) * keep
    rows = dot(group, spread.astype(BF16)) + fill
    comb[...] = rows
    nq[...] = xq[...].astype(BF16)
    pay[0:160, :] = xq[0].astype(BF16)
    pay[160:320, :] = xq[5].astype(BF16)
    last = jnp.concatenate([rows[2:3, 0:256], rows[2:3, 256:512], jnp.zeros((14, 256), F32)], axis=0)
    pay[320:336, 0:256] = last.astype(BF16)
    copies[2].wait()
    for c in range(CHUNKS):
        own[c] = jnp.concatenate([spread_table(eb.at[2], c), jnp.zeros((4, 256), F32)], axis=0)
        pay[336 + 16 * c:352 + 16 * c, 0:256] = own[c].astype(BF16)
        inner[c, 0:12, :] = spread_table(eb.at[0], c)
        inner[c, 12:24, :] = spread_table(eb.at[1], c)
    for copy in copies[3:]:
        copy.wait()
    pick, place, tile, keep, gather = bufs
    idx = index[...]
    for part, m_ref, r_ref in ((idx & 255, lo_m, lo_r), (idx >> 8, hi_m, hi_r)):
        picked = dot(pick[...], part.astype(F32).astype(BF16)).astype(BF16)
        full = dot(picked, place[...])
        m_ref[...] = full[:, 0:128]
        wide = dot(full[:, 128:144].astype(BF16), tile[...]) * keep[...]
        r_ref[...] = dot(gather[...], wide.astype(BF16))


def column(nq, lat, scr, cs):
    sl = slice(40 * cs, 40 * cs + 40)
    scr[0:40, :] = lat[160:320, :].astype(F32)[sl, :]
    scr[280:320, :] = lat[0:160, :].astype(F32)[sl, :]
    for rt in range(6):
        scr[40 * rt + 40:40 * rt + 80, :] = nq[rt].astype(F32)[sl, :]
    return scr[...].astype(BF16)


def right_body(nq, lat, comb, pay, scr):
    pay[0:320, :] = column(nq, lat, scr, 3)
    top = lat[320:336, 0:256].astype(F32)
    rows = jnp.concatenate([top[1:2, :], comb[0:3, 256:512], jnp.zeros((12, 256), F32)], axis=0)
    pay[320:336, 0:256] = rows.astype(BF16)


def left_body(nq, lat, after, pay, scr):
    pay[...] = column(nq, lat, scr, 0)


def block_range(stage):
    lon = lax.axis_index("lon")
    first = jnp.where((lon == 0) & (lax.axis_index("lat") == 1) & (lax.axis_index("ens") == 0), 4, 0)
    second = jnp.where(lon % 32 == 31, 0, jnp.maximum(first, 2))
    behind = (lon == 0) & (lax.axis_index("lat") == 0) & (lax.axis_index("ens") == 0)
    third = jnp.where(behind, 4, jnp.maximum(second, 8 - lon % 32))
    return ((0, first), (first, second), (second, third), (third, 8))[stage]


def bias_body(stage, lo_m, hi_m, lo_r, hi_r, own, inner, swap, *refs):
    main0, rem0, main1, rem1, tabs = (refs[0:4] + refs[-1:]) if stage == 0 else refs[-5:]
    begin, end = block_range(stage)
    low = lax.broadcasted_iota(jnp.int32, (256, 256), 0).astype(F32)

    def look(table, lo, hi):
        hot = jnp.where(low == lo, 1.0, 0.0).astype(BF16)
        got = dot(table, hot)
        out = got[0:ROWS]
        for c in range(1, CHUNKS):
            out = jnp.where(hi == float(c), got[ROWS * c:ROWS * c + ROWS], out)
        return out * LOG2E

    for c in range(CHUNKS):
        tabs[ROWS * c + 16:ROWS * c + ROWS, :] = inner[c]

    for half, main, rem in ((0, main0, rem0), (1, main1, rem1))[:1 if stage < 2 else 2]:
        for c in range(CHUNKS):
            tabs[ROWS * c:ROWS * c + 16, :] = \
                swap[336 + 16 * c:352 + 16 * c, 0:256].astype(F32) if half else own[c]
        table = tabs[...].astype(BF16)

        def pairs(block, carry):
            first = 24 * block
            for step in range(12):
                at = 72 * half + first + 2 * step
                lo = jnp.concatenate([lo_m[pl.ds(at, 1), :], lo_m[pl.ds(at + 1, 1), :]], axis=1)
                hi = jnp.concatenate([hi_m[pl.ds(at, 1), :], hi_m[pl.ds(at + 1, 1), :]], axis=1)
                out = look(table, lo, hi)
                spot = first + 2 * step
                spot = spot + jnp.where(spot >= 36, 4, 0)
                main[pl.ds(spot, ROWS, stride=SPAN), :] = out[:, 0:128]
                main[pl.ds(spot + 1, ROWS, stride=SPAN), :] = out[:, 128:256]
            return carry

        lax.fori_loop(jnp.clip(begin - 4 * half, 0, 3), jnp.clip(end - 4 * half, 0, 3), pairs, 0)

        @pl.when((begin <= 4 * half + 3) & (end > 4 * half + 3))
        def _():
            for g in range(5):
                out = look(table, lo_r[8 * half + g:8 * half + g + 1, :], hi_r[8 * half + g:8 * half + g + 1, :])
                for q in range(min(16, 72 - 16 * g)):
                    i = 16 * g + q
                    spot = i + 4 * (i // 36)
                    piece = out[:, 128 * (q // 8):128 * (q // 8) + 128]
                    if q % 8:
                        piece = pltpu.roll(piece, 128 - 16 * (q % 8), axis=1)
                    rem[pl.ds(spot, ROWS, stride=SPAN), :] = piece


SPANS = ((40, 40, 0), (0, 80, 40), (0, 40, 120))
SCALE = 32 ** -0.5 * LOG2E


def head_lanes():
    lane = lax.broadcasted_iota(jnp.int32, (1, 128), 1)
    return lane, [(lane // 32 == h) for h in range(4)]


def put(xs, group, rt, second, block):
    at = 576 * group + 72 * rt + 36 * second
    xs[at:at + 36, :] = block[0:36, :]


def key_values(xs, kk, vv, w_qkv, count):
    def project(step, carry):
        at = pl.multiple_of(step * 288, 288)
        y = dot(xs[pl.ds(at, 288), :].astype(BF16), w_qkv[:, C:3 * C])
        kk[pl.ds(at, 288), :] = y[:, 0:C].astype(BF16)
        vv[pl.ds(at, 288), :] = y[:, C:2 * C].astype(BF16)
        return carry

    lax.fori_loop(0, count, project, 0, unroll=count)


def region_features(rows, qf, kf):
    sub = lax.broadcasted_iota(jnp.int32, (8, KEYS), 0).astype(F32)
    hot = jnp.concatenate([jnp.where(sub == rows[n:n + 1, 0:KEYS], 1.0, 0.0) for n in range(8)], axis=0)
    eye = lax.broadcasted_iota(jnp.int32, (64, 128), 0) == lax.broadcasted_iota(jnp.int32, (64, 128), 1)
    seen = lax.dot_general(
        jnp.concatenate([hot, jnp.zeros((64, KEYS), F32)], axis=0).astype(BF16),
        jnp.concatenate([jnp.where(eye, 1.0, 0.0), jnp.zeros((64, 128), F32)], axis=0).astype(BF16),
        (((0,), (0,)), ((), ())), preferred_element_type=F32)
    qf[...] = jnp.zeros((160, 128), F32)
    for n in range(4):
        qf[40 * n:40 * n + 36, :] = seen[36 * n:36 * n + 36, :]
    kf[...] = (seen - 1.0) * 1e30


def attention(windows, tables, qq, kk, vv, qf, kf, sc, mx, store):
    lane, heads = head_lanes()
    ones = jnp.ones((KEYS, 128), BF16)

    def places(r2, step):
        return (step, 2 * step + 1) if r2 else (step + 1, 2 * step + 2)

    def score(r2, step):
        t, rt = places(r2, step)
        if r2:
            th0 = jnp.where(step == 0, 0, 4 + 12 * step)
        else:
            th0 = jnp.where(step == 2, 0, 16 + 12 * step)
        bm, br = tables[r2]
        top = 0
        for n, w in enumerate(windows):
            c0, nrow, q0 = SPANS[w]
            far = jnp.where(lane // 8 == 4 * n + t, kf[...], 0.0).astype(BF16)
            near = qf[80 * r2 + c0:80 * r2 + c0 + nrow, :]
            for g in range(3):
                sl = slice(128 * g, 128 * g + 128)
                k = jnp.concatenate([kk[pl.ds(pl.multiple_of(576 * n + 144 * t, 144), KEYS), sl], far], axis=1)
                q = qq[rt - 1, q0:q0 + nrow, sl]
                qs = jnp.concatenate([jnp.concatenate([jnp.where(m, q, 0.0), near], axis=1) for m in heads],
                                     axis=0).astype(BF16)
                s = lax.dot_general(qs, k, (((1,), (1,)), ((), ())), preferred_element_type=F32)
                for h in range(4):
                    th = pl.multiple_of((th0 + 4 * g + h) * SPAN, SPAN) + c0
                    b = jnp.concatenate([bm[pl.ds(th, nrow), :], br[pl.ds(th, nrow), :][:, 0:16]], axis=1)
                    x = s[h * nrow:(h + 1) * nrow, :] * SCALE + b
                    sc[r2, top:top + nrow, :] = x
                    mx[r2, top:top + nrow, :] = jnp.broadcast_to(jnp.max(x, axis=1, keepdims=True), (nrow, 128))
                    top += nrow

    def attend(r2, step):
        t, rt = places(r2, step)
        top = 0
        for n, w in enumerate(windows):
            _, nrow, _ = SPANS[w]
            for g in range(3):
                sl = slice(128 * g, 128 * g + 128)
                parts = []
                for _ in range(4):
                    m = mx[r2, top:top + nrow, :]
                    x = sc[r2, top:top + nrow, :] - jnp.concatenate([m, m[:, 0:16]], axis=1)
                    parts.append(jnp.exp2(x).astype(BF16))
                    top += nrow
                v = vv[pl.ds(pl.multiple_of(576 * n + 144 * t, 144), KEYS), sl]
                o = dot(jnp.concatenate(parts, axis=0), jnp.concatenate([v, ones], axis=1))
                os = [o[h * nrow:(h + 1) * nrow, :] for h in range(4)]
                num, den = os[3][:, 0:128], os[3][:, 128:256]
                for h in range(3):
                    num = jnp.where(heads[h], os[h][:, 0:128], num)
                    den = jnp.where(heads[h], os[h][:, 128:256], den)
                store(rt - 1, w, sl, num / den)

    score(0, 0)

    def steps(step, carry):
        score(1, step)
        attend(0, step)
        score(0, jnp.minimum(step + 1, 2))
        attend(1, step)
        return carry

    lax.fori_loop(0, 3, steps, 0)


def inner_body(nq, lat, comb, bm1, br1, bm0, br0, w_qkv, qq, ctx, xs, kk, vv, rows, qf, kf, sc, mx):
    for rt in range(8):
        block = lat[160:320, :] if rt == 0 else lat[0:160, :] if rt == 7 else nq[rt - 1]
        block = block.astype(F32)
        put(xs, 0, rt, 0, block[40:80, :])
        put(xs, 0, rt, 1, block[80:120, :])
    key_values(xs, kk, vv, w_qkv, 2)
    for rt in range(6):
        qq[rt] = dot(nq[rt], w_qkv[:, 0:C]).astype(BF16).astype(F32)
    rows[...] = jnp.full((8, 256), -1.0, F32)
    rows[0:1, :] = lat[320:336, 0:256].astype(F32)[0:1, :]
    rows[1:4, :] = comb[0:3, 0:256]
    region_features(rows, qf, kf)

    def store(rt, w, sl, value):
        ctx[rt, :, sl] = value

    attention((1,), ((bm0, br0), (bm1, br1)), qq, kk, vv, qf, kf, sc, mx, store)


def outer_body(fields, nq, lat, left, right, comb, qq, mid, bm1, br1, bm0, br0, w_qkv, w_proj, w_fc1, w_fc2, out,
               xs, kk, vv, ctx, att, rows, res, qf, kf, sc, mx):
    below = lat[0:160, :].astype(F32)
    above = lat[160:320, :].astype(F32)
    put(xs, 0, 0, 1, above[0:40, :])
    put(xs, 1, 0, 0, above[120:160, :])
    put(xs, 0, 7, 1, below[0:40, :])
    put(xs, 1, 7, 0, below[120:160, :])
    lhalo = left[0:320, :].astype(F32)
    rhalo = right[...].astype(F32)
    for rt in range(8):
        put(xs, 0, rt, 0, lhalo[40 * rt:40 * rt + 40, :])
        put(xs, 1, rt, 1, rhalo[40 * rt:40 * rt + 40, :])
    for rt in range(6):
        own = nq[rt].astype(F32)
        put(xs, 0, rt + 1, 1, own[0:40, :])
        put(xs, 1, rt + 1, 0, own[120:160, :])
        ctx[rt, 40:120, :] = mid[rt]
    key_values(xs, kk, vv, w_qkv, 4)
    rows[0:4, :] = left[320:336, 0:256].astype(F32)[0:4, :]
    rows[4:5, :] = lat[320:336, 0:256].astype(F32)[1:2, :]
    rows[5:8, :] = comb[0:3, 256:512]
    region_features(rows, qf, kf)

    def store(rt, w, sl, value):
        ctx[rt, SPANS[w][2]:SPANS[w][2] + 40, sl] = value

    attention((0, 2), ((bm0, br0), (bm1, br1)), qq, kk, vv, qf, kf, sc, mx, store)

    def back(rt, carry):
        att[rt] = dot(ctx[rt].astype(BF16), w_proj[...]).astype(BF16).astype(F32)
        for level in range(2):
            for r3 in range(3):
                base = 6 * ((1 - level) * 3 + r3)
                for cs in range(4):
                    res[level * 18 + 3 * rt + r3, 6 * cs:6 * cs + 6, :] = \
                        att[rt, 40 * cs + base:40 * cs + base + 6, :]
        return carry

    lax.fori_loop(0, 6, back, 0, unroll=6)

    def feed(step, carry):
        x = fields[pl.ds(9 * step, 9)].astype(F32) + res[pl.ds(9 * step, 9)]
        x = x.reshape(216, C).astype(BF16).astype(F32)
        y = dot(normalise(x), w_fc1[...])
        hidden = (0.5 * y * (1.0 + lax.erf(y * (0.5 ** 0.5)))).astype(BF16)
        z = x + dot(hidden, w_fc2[...])
        out[pl.ds(9 * step, 9)] = z.reshape(9, 24, C).astype(BF16)
        return carry

    lax.fori_loop(0, 4, feed, 0, unroll=4)


def call(body, outs, scratch, args, limit=28, **kw):
    return pl.pallas_call(
        body,
        out_shape=outs,
        scratch_shapes=scratch,
        compiler_params=pltpu.CompilerParams(vmem_limit_bytes=limit << 20),
        **kw,
    )(*args)


def hold(x):
    return pltpu.with_memory_space_constraint(x, pltpu.HBM)


def shift(value, axis, steps):
    count = lax.axis_size(axis)
    return lax.ppermute(value, axis, [(s, (s + steps) % count) for s in range(count)])


def sds(shape, dtype):
    return jax.ShapeDtypeStruct(shape, dtype)


def local(fields, region_ids, bias_index, earth_bias, w_qkv, w_proj, w_fc1, w_fc2):
    fields = fields.reshape(36, 24, C)
    region = region_ids.transpose(1, 0, 2)
    tables = earth_bias.transpose(0, 2, 1)
    vm = pltpu.VMEM
    kinds = (BF16, BF16, BF16, F32, BF16)
    consts = tuple(jnp.asarray(c, k) for c, k in zip(index_constants(), kinds))
    nq, comb, pay, own, *found, inner = call(
        prep_body,
        (sds((6, 160, C), BF16), sds((8, 512), F32), sds((544, C), BF16), sds((CHUNKS, 16, 256), F32),
         sds((144, 128), F32), sds((144, 128), F32), sds((16, 256), F32), sds((16, 256), F32),
         sds((CHUNKS, 24, 256), F32)),
        [vm((6, 160, C), F32), vm((36, 24), F32), vm((36, 24, C), BF16), vm((18, 2, 24), jnp.int32),
         vm((3, HEADS, POSITIONS), BF16), vm((144, 144), jnp.int32)] +
        [vm(c.shape, c.dtype) for c in consts] + [pltpu.SemaphoreType.DMA((9,))],
        tuple(hold(x) for x in (fields, region, tables, bias_index) + consts),
        in_specs=[pl.BlockSpec(memory_space=pltpu.HBM)] * 9,
    )

    def bias(stage, extra, kept, also=()):
        count = len(kept) + len(also)
        table = (sds((ROWS * SPAN, 128), F32),) * 4
        alias = {7 + n: n for n in range(4)} if stage else {7: 4}
        return call(
            lambda *refs: bias_body(stage, *refs[:7], *refs[7 + count:]),
            table if stage else table + (sds(pay.shape, pay.dtype),),
            [vm((CHUNKS * ROWS, 256), F32)],
            tuple(found) + (own, inner, extra) + kept + also,
            in_specs=[pl.BlockSpec(memory_space=vm)] * 7 + [pl.BlockSpec(memory_space=vm if stage else pl.ANY)] * count,
            out_specs=tuple([pl.BlockSpec(memory_space=vm)] * 4 + [pl.BlockSpec(memory_space=pl.ANY)] * (not stage)),
            cost_estimate=pl.CostEstimate(flops=10 ** 10 if stage > 1 else 3 * 10 ** 9, transcendentals=0,
                                          bytes_accessed=8 * 10 ** 6),
            input_output_aliases=alias,
        )

    *some, pay = bias(0, own, (pay,))
    lat = shift(pay, "lat", 1)
    some = bias(1, own, tuple(some))
    pay_r = call(right_body, sds((336, C), BF16), [pltpu.VMEM((320, C), F32)], (nq, lat, comb))
    left = shift(pay_r, "lon", 1)
    some = bias(2, lat, tuple(some), (w_qkv,))
    pay_l = call(
        left_body,
        sds((320, C), BF16),
        [pltpu.VMEM((320, C), F32)],
        (nq, lat, some[0]),
        in_specs=[pl.BlockSpec(memory_space=pltpu.VMEM)] * 2 + [pl.BlockSpec(memory_space=pl.ANY)],
    )
    right = shift(pay_l, "lon", -1)
    bm0, br0, bm1, br1 = bias(3, lat, tuple(some))
    vm = pltpu.VMEM
    work = [vm((8, 256), F32), vm((160, 128), F32), vm((KEYS, 128), F32)]
    qq, mid = call(
        inner_body,
        (sds((6, 160, C), F32), sds((6, SPAN, C), F32)),
        [vm((576, C), F32), vm((576, C), BF16), vm((576, C), BF16)] + work +
        [vm((2, 960, KEYS), F32), vm((2, 960, 128), F32)],
        (nq, lat, comb, bm1, br1, bm0, br0, w_qkv),
        cost_estimate=pl.CostEstimate(flops=5 * 10 ** 9, transcendentals=0, bytes_accessed=8 * 10 ** 6),
    )
    result = call(
        outer_body,
        sds((36, 24, C), BF16),
        [vm((1152, C), F32), vm((1152, C), BF16), vm((1152, C), BF16), vm((6, 160, C), F32), vm((6, 160, C), F32),
         work[0], vm((36, 24, C), F32)] + work[1:] + [vm((2, 960, KEYS), F32), vm((2, 960, 128), F32)],
        (fields, nq, lat, left, right, comb, qq, mid, bm1, br1, bm0, br0, w_qkv, w_proj, w_fc1, w_fc2),
    )
    return result.reshape(2, 18, 24, C)


def solution(mesh):
    return jax.shard_map(
        local,
        mesh=mesh,
        in_specs=(
            P("ens", "lat", "lon", None),
            P(None, "lat", "lon"),
            P(),
            P("lat", None, None),
            P(),
            P(),
            P(),
            P(),
        ),
        out_specs=P("ens", "lat", "lon", None),
        check_vma=False,
    )
```
